32 devices in a mesh: genome: 16 (over z, x, core), samples: 2 (over y).
Axes of the slice: x: 2, y: 2, z: 4, core: 2. Of those that a mesh axis runs over, the one named last changes fastest.
Arguments:
- haplotypes: bfloat16 [4096, 16384], P('samples', 'genome'), may hold values from 0 to 1
- window_ends: int32 [16384], P(('genome', 'samples')), may hold values from 1 to 16384, as said below
Outputs:
- ld_score: float32 [16384], P(('genome', 'samples'))
- profile: float32 [2, 16384], P(None, ('genome', 'samples'))
The draws below stay inside these ranges and needn't reach their ends.
Inputs may be any that keep to these rules, and one draw needn't show every extreme that they name: window_ends[v] - v lies between 1 and 1024 for every variant v, and equals 1024 at v = 0.
All inputs are finite; a program needn't handle non-finite values.
Results may differ from the reference program's by a relative error of at most 0.0013.
Values may be sent and summed in bfloat16 or wider, within the bound.
No kernel may reach another device: no remote copies, remote signals or barrier semaphores. Data moves between devices by JAX's collectives and lax.ppermute only.
A program may use at most 64 MiB of HBM per device.

```python
import math
import jax
import jax.numpy as jnp
from jax import lax

HAP_DEV = 2048
WIN = 1024
TILE = 128
HAPLOS = 4096
VARIANTS = 16384
SHARE = 512


def smooth_curve(curve_key, row_count, spacing):
    knot_count = VARIANTS // spacing + 3
    knot_key, offset_key = jax.random.split(curve_key)
    knots = jax.random.normal(knot_key, (row_count, knot_count), jnp.float32)
    offsets = jax.random.randint(offset_key, (row_count, 1), 0, spacing)
    placed = jnp.arange(VARIANTS, dtype=jnp.int32)[None, :] + offsets
    left_index = placed // spacing
    fraction = (placed % spacing).astype(jnp.float32) / float(spacing)
    lower = jnp.take_along_axis(knots, left_index, axis=1)
    upper = jnp.take_along_axis(knots, left_index + 1, axis=1)
    return lower * (1.0 - fraction) + upper * fraction


def draw_haplotypes(key, part):
    block_rows = min(HAP_DEV, 256)
    block_total = HAPLOS // block_rows
    threshold = jax.random.uniform(jax.random.fold_in(key, 11), (VARIANTS,), jnp.float32, -1.0, 3.0)
    coarse_space = 4 * WIN
    middle_space = max(WIN // 2, 2)
    fine_space = max(WIN // 16, 2)

    def sample_block(block_index):
        block_key = jax.random.fold_in(jax.random.fold_in(key, 23), block_index)
        sub_keys = jax.random.split(block_key, 4)
        latent = smooth_curve(sub_keys[0], block_rows, coarse_space)
        latent = latent + 0.5 * smooth_curve(sub_keys[1], block_rows, middle_space)
        latent = latent + 0.3 * smooth_curve(sub_keys[2], block_rows, fine_space)
        noise = jax.random.normal(sub_keys[3], (block_rows, VARIANTS), jnp.float32)
        return jax.nn.sigmoid(3.0 * (latent - threshold[None, :]) + noise)
    dosage = lax.map(sample_block, jnp.arange(block_total, dtype=jnp.int32)).reshape(HAPLOS, VARIANTS)
    return dosage.astype(jnp.bfloat16)


def draw_window_ends(key, part):
    spans = jax.random.randint(jax.random.fold_in(key, 37), (VARIANTS,), 1, WIN + 1)
    spans = spans.at[0].set(WIN)
    return jnp.minimum(jnp.arange(VARIANTS, dtype=jnp.int32) + spans, VARIANTS).astype(jnp.int32)


def setup_inputs(seed: int = 0) -> dict:
    key_of = jax.random.split(jax.random.key(seed), 3)
    return {
        "haplotypes": draw_haplotypes(jax.random.fold_in(key_of[2], 71), 0),
        "window_ends": draw_window_ends(jax.random.fold_in(key_of[2], 71), 0),
    }


variance_floor = 0.01

def standardize(alleles, frequency, inverse_sd):
    return ((alleles.astype(jnp.float32) - frequency) * inverse_sd).astype(jnp.bfloat16)

def transpose_product(left_side, right_side):
    return lax.dot_general(left_side, right_side, (((0,), (0,)), ((), ())), preferred_element_type=jnp.float32)

def window_mean(cross_sum, haplo_total, row_position, column_position, window_end):
    correlation = cross_sum / haplo_total
    inside = (column_position > row_position[:, None]) & (column_position < window_end[:, None])
    squares = lax.optimization_barrier(jnp.sum(jnp.where(inside, correlation * correlation, jnp.zeros_like(correlation)), axis=1))
    counted = jnp.maximum(window_end - row_position - 1, 1).astype(jnp.float32)
    return squares / counted

def reference(haplotypes, window_ends):
    haplo_total = float(haplotypes.shape[0])
    variants = haplotypes.shape[1]
    counts = lax.optimization_barrier(jnp.sum(haplotypes, axis=0, dtype=jnp.float32))
    frequency = counts / haplo_total
    inverse_sd = lax.rsqrt(jnp.maximum(frequency * (1.0 - frequency), variance_floor))
    padded_haps = jnp.pad(haplotypes, ((0, 0), (0, WIN)))
    padded_freq = jnp.pad(frequency, (0, WIN))
    padded_isd = jnp.pad(inverse_sd, (0, WIN))

    def tile_scores(tile_index):
        first_row = tile_index * TILE
        columns = lax.dynamic_slice_in_dim(padded_haps, first_row, TILE + WIN, 1)
        standard = standardize(columns, lax.dynamic_slice_in_dim(padded_freq, first_row, TILE + WIN), lax.dynamic_slice_in_dim(padded_isd, first_row, TILE + WIN))
        cross_sum = transpose_product(standard[:, :TILE], standard)
        row_position = first_row + jnp.arange(TILE, dtype=jnp.int32)
        column_position = jnp.broadcast_to(first_row + jnp.arange(TILE + WIN, dtype=jnp.int32)[None, :], (TILE, TILE + WIN))
        window_end = lax.dynamic_slice_in_dim(window_ends, first_row, TILE)
        return window_mean(cross_sum, haplo_total, row_position, column_position, window_end)
    ld_score = lax.map(tile_scores, jnp.arange(variants // TILE, dtype=jnp.int32)).reshape(variants)
    log_rates = jnp.array([math.log(0.5) / (4 * SHARE), math.log(0.1) / variants], jnp.float32)
    decay = jnp.exp(log_rates)

    def advance(state, value):
        state = decay * state + value
        return (state, state)
    _, smoothed = lax.scan(advance, jnp.zeros(2, jnp.float32), ld_score)
    position = jnp.arange(variants, dtype=jnp.float32) + 1.0
    profile = smoothed.T * (-jnp.expm1(log_rates))[:, None] / -jnp.expm1(position[None, :] * log_rates[:, None])
    return (ld_score, profile)
```

```python
import functools
import math

import jax
import jax.numpy as jnp
from jax import lax
from jax.experimental import pallas as pl
from jax.experimental.pallas import tpu as pltpu
from jax.sharding import PartitionSpec as P

WIN = 1024
LANES = 128
CHUNKS = 4
STEP = 512
variance_floor = 0.01


def standardize(alleles, frequency, inverse_sd):
    return ((alleles.astype(jnp.float32) - frequency) * inverse_sd).astype(jnp.bfloat16)


def product(left, right):
    return lax.dot_general(
        left, right, (((0,), (0,)), ((), ())), preferred_element_type=jnp.float32
    )


def moments(counts, haplo_total):
    frequency = counts / haplo_total
    return frequency, lax.rsqrt(jnp.maximum(frequency * (1.0 - frequency), variance_floor))


def owner_spans(first, width, share):
    spans = []
    for owner in range(width // share):
        lo, hi = max(first, owner * share), (owner + 1) * share
        if lo < hi:
            spans.append((owner, lo, hi))
    return spans


def own_kernel(share, haplo_total, hap_ref, counts_ref, std_ref, *outs):
    step = pl.program_id(0)
    width = hap_ref.shape[1]
    frequency, inverse_sd = moments(counts_ref[...], haplo_total)
    std = standardize(hap_ref[...], frequency, inverse_sd)
    std_ref[...] = std
    owners = width // share
    keeps, sends = outs[:owners], outs[owners:]
    block = min(256, share)
    for owner in range(owners):
        keep = keeps[owner]
        base = owner * share
        for col in range(base, base + share, block):
            part = product(std[:, col:], std[:, col : col + block])
            place = (slice(col - base, width - base), slice(col - base, col - base + block))

            @pl.when(step == 0)
            def _(keep=keep, place=place, part=part, col=col, base=base):
                keep[place] = part
                if col > base:
                    keep[: col - base, place[1]] = jnp.zeros((col - base, block), jnp.float32)

            @pl.when(step > 0)
            def _(keep=keep, place=place, part=part):
                keep[place] += part

    @pl.when(step == pl.num_programs(0) - 1)
    def _():
        for keep, send in zip(keeps, sends):
            send[...] = keep[...].astype(jnp.bfloat16)


def own_products(haplotypes, counts, share, haplo_total):
    depth, width = haplotypes.shape
    owners = width // share
    shapes = [(width - owner * share, share) for owner in range(owners)]
    return pl.pallas_call(
        functools.partial(own_kernel, share, haplo_total),
        grid=(depth // STEP,),
        in_specs=[
            pl.BlockSpec((STEP, width), lambda k: (k, 0)),
            pl.BlockSpec((1, width), lambda k: (0, 0)),
        ],
        out_specs=[pl.BlockSpec((STEP, width), lambda k: (k, 0))]
        + [pl.BlockSpec(s, lambda k: (0, 0)) for s in shapes] * 2,
        out_shape=[jax.ShapeDtypeStruct((depth, width), jnp.bfloat16)]
        + [jax.ShapeDtypeStruct(s, jnp.float32) for s in shapes]
        + [jax.ShapeDtypeStruct(s, jnp.bfloat16) for s in shapes],
        name="own_products",
    )(haplotypes, counts)


def chunk_kernel(spans, first, haplo_total, raw_ref, counts_ref, std_ref, *outs):
    step = pl.program_id(0)
    frequency, inverse_sd = moments(counts_ref[...], haplo_total)
    std = standardize(raw_ref[...], frequency, inverse_sd)
    keeps, sends = outs[: len(spans)], outs[len(spans) :]
    for keep, (_, lo, hi) in zip(keeps, spans):
        part = product(std, std_ref[:, lo - first : hi - first])

        @pl.when(step == 0)
        def _(keep=keep, part=part):
            keep[...] = part

        @pl.when(step > 0)
        def _(keep=keep, part=part):
            keep[...] += part

    @pl.when(step == pl.num_programs(0) - 1)
    def _():
        for keep, send in zip(keeps, sends):
            send[...] = keep[...].astype(jnp.bfloat16)


def chunk_products(raw, counts, standard, first, share, haplo_total):
    depth, width = raw.shape
    total = standard.shape[1]
    spans = owner_spans(first, total, share)
    step = STEP
    shapes = [(width, hi - lo) for _, lo, hi in spans]
    return pl.pallas_call(
        functools.partial(chunk_kernel, spans, 0, haplo_total),
        grid=(depth // step,),
        in_specs=[
            pl.BlockSpec((step, width), lambda k: (k, 0)),
            pl.BlockSpec((1, width), lambda k: (0, 0)),
            pl.BlockSpec((step, total), lambda k: (k, 0)),
        ],
        out_specs=[pl.BlockSpec(s, lambda k: (0, 0)) for s in shapes] * 2,
        out_shape=[jax.ShapeDtypeStruct(s, jnp.float32) for s in shapes]
        + [jax.ShapeDtypeStruct(s, jnp.bfloat16) for s in shapes],
        name=f"chunk_products_{first}",
    )(raw, counts, standard), spans


def combine_kernel(spans, share, first_column, first_row, haplo_total, place, ends_ref, before_ref, *rest):
    n = len(spans)
    keeps, gots, out_ref = rest[:n], rest[n : 2 * n], rest[2 * n]
    out_ref[...] = before_ref[...]
    for keep, got, (owner, lo, hi), top in zip(keeps, gots, spans, first_row):

        @pl.when(place[0] == owner)
        def _(keep=keep, got=got, owner=owner, lo=lo, hi=hi, top=top):
            inner = slice(lo - owner * share, hi - owner * share)
            ends = ends_ref[:, inner]
            total = (keep[...] + got[...].astype(jnp.float32)) / haplo_total
            column = first_column + top + lax.broadcasted_iota(jnp.int32, total.shape, 0)
            row = lo + lax.broadcasted_iota(jnp.int32, total.shape, 1)
            inside = (column > row) & (column < ends)
            sums = jnp.sum(jnp.where(inside, total * total, 0.0), axis=0, keepdims=True)
            out_ref[:, inner] += sums


def combine(keeps, gots, spans, tops, first_column, ends, before, place, share, haplo_total):
    return pl.pallas_call(
        functools.partial(combine_kernel, spans, share, first_column, tops, haplo_total),
        in_specs=[pl.BlockSpec(memory_space=pltpu.SMEM)]
        + [pl.BlockSpec(memory_space=pltpu.VMEM)] * (2 + 2 * len(spans)),
        out_specs=pl.BlockSpec(memory_space=pltpu.VMEM),
        out_shape=jax.ShapeDtypeStruct((1, share), jnp.float32),
        name=f"combine_{first_column}",
    )(place, ends, before, *keeps, *gots)


def rates_of(share, variants):
    return (math.log(0.5) / (4 * share), math.log(0.1) / variants)


def local_kernel(rates, place, ends_ref, sums_ref, score_ref, local_ref, last_ref):
    share = ends_ref.shape[1]
    row = place[0] * share + lax.broadcasted_iota(jnp.int32, (1, share), 1)
    counted = jnp.maximum(ends_ref[...] - row - 1, 1).astype(jnp.float32)
    score = sums_ref[...] / counted
    score_ref[...] = score
    blocks = share // LANES
    stacked = jnp.concatenate(
        [score[:, b * LANES : (b + 1) * LANES] for b in range(blocks)]
        + [jnp.zeros(((-blocks) % 8, LANES), jnp.float32)] * (1 if blocks % 8 else 0),
        axis=0,
    )
    source = lax.broadcasted_iota(jnp.int32, (LANES, LANES), 0)
    target = lax.broadcasted_iota(jnp.int32, (LANES, LANES), 1)
    lag = (target - source).astype(jnp.float32)
    lane = lax.broadcasted_iota(jnp.int32, (1, LANES), 1).astype(jnp.float32)
    lasts = []
    for k, rate in enumerate(rates):
        weight = jnp.where(lag >= 0.0, jnp.exp(jnp.maximum(lag, 0.0) * rate), 0.0)
        inner = lax.dot_general(
            stacked,
            weight,
            (((1,), (0,)), ((), ())),
            precision=lax.Precision.HIGHEST,
            preferred_element_type=jnp.float32,
        )
        fall = jnp.exp((lane + 1.0) * rate)
        carry = jnp.zeros((1, 1), jnp.float32)
        for b in range(blocks):
            here = inner[b : b + 1, :] + carry * fall
            local_ref[k : k + 1, b * LANES : (b + 1) * LANES] = here
            carry = here[:, LANES - 1 :]
        lasts.append(carry)
    tile_lane = lax.broadcasted_iota(jnp.int32, last_ref.shape, 1)
    last_ref[...] = jnp.where(tile_lane == 0, lasts[0], jnp.where(tile_lane == 1, lasts[1], 0.0))


def local_sums(ends, sums, place, rates, peers):
    share = ends.shape[1]
    return pl.pallas_call(
        functools.partial(local_kernel, rates),
        in_specs=[pl.BlockSpec(memory_space=pltpu.SMEM)]
        + [pl.BlockSpec(memory_space=pltpu.VMEM)] * 2,
        out_specs=[pl.BlockSpec(memory_space=pltpu.VMEM)] * 3,
        out_shape=[
            jax.ShapeDtypeStruct((1, share), jnp.float32),
            jax.ShapeDtypeStruct((2, share), jnp.float32),
            jax.ShapeDtypeStruct((peers, LANES), jnp.float32),
        ],
        name="local_sums",
    )(place, ends, sums)


def finish_kernel(rates, place, local_ref, table_ref, norm_ref, profile_ref):
    share = local_ref.shape[1]
    peers = table_ref.shape[0]
    me = place[1]
    peer = lax.broadcasted_iota(jnp.int32, (peers, LANES), 0)
    gap = ((me - 1 - peer) * share).astype(jnp.float32)
    step = lax.broadcasted_iota(jnp.int32, (1, share), 1).astype(jnp.float32)
    for k, rate in enumerate(rates):
        weight = jnp.where(peer < me, jnp.exp(jnp.maximum(gap, 0.0) * rate), 0.0)
        incoming = jnp.sum(weight * table_ref[...], axis=0, keepdims=True)[:, k : k + 1]
        smoothed = local_ref[k : k + 1, :] + incoming * jnp.exp((step + 1.0) * rate)
        profile_ref[k : k + 1, :] = smoothed * norm_ref[k : k + 1, :]


def finish(local, table, norm, place, rates):
    return pl.pallas_call(
        functools.partial(finish_kernel, rates),
        in_specs=[pl.BlockSpec(memory_space=pltpu.SMEM)]
        + [pl.BlockSpec(memory_space=pltpu.VMEM)] * 3,
        out_specs=pl.BlockSpec(memory_space=pltpu.VMEM),
        out_shape=jax.ShapeDtypeStruct(local.shape, jnp.float32),
        name="finish",
    )(place, local, table, norm)


def per_device(haplotypes, window_ends):
    samples = lax.axis_size("samples")
    genome = lax.axis_size("genome")
    width = haplotypes.shape[1]
    share = width // samples
    haplo_total = float(haplotypes.shape[0] * samples)
    sample_index = lax.axis_index("samples")
    genome_index = lax.axis_index("genome")
    place = jnp.stack([sample_index, genome_index * samples + sample_index]).astype(jnp.int32)
    back = [(i + 1, i) for i in range(genome - 1)]
    size = width // CHUNKS

    def hand(send, owner):
        return lax.ppermute(send, "samples", [(1 - owner, owner)])

    raws = [
        lax.ppermute(haplotypes[:, c * size : (c + 1) * size], "genome", back)
        for c in range(CHUNKS)
    ]
    counts = jnp.sum(haplotypes, axis=0, dtype=jnp.float32)[None]
    if samples == 2:
        counts = counts + lax.ppermute(counts, "samples", [(0, 1), (1, 0)])
    else:
        counts = lax.psum(counts, "samples")
    next_counts = lax.ppermute(counts, "genome", back)
    ends = (window_ends - genome_index * width)[None]

    def gather(keeps, sends, spans, tops, first_column, before):
        if samples == 2:
            gots = [hand(send, owner) for send, (owner, _, _) in zip(sends, spans)]
            return combine(keeps, gots, spans, tops, first_column, ends, before, place, share, haplo_total)
        sums = before
        for keep, (owner, lo, hi), top in zip(keeps, spans, tops):
            total = lax.psum(keep, "samples")
            sums = combine([total], [jnp.zeros_like(total)], [(owner, lo, hi)], [top], first_column, ends, sums, place, share, haplo_total)
        return sums

    out = own_products(haplotypes, counts, share, haplo_total)
    standard, keeps, sends = out[0], out[1 : 1 + samples], out[1 + samples :]
    spans = owner_spans(0, width, share)
    sums = gather(keeps, sends, spans, [lo for _, lo, _ in spans], 0, jnp.zeros((1, share), jnp.float32))
    for c in range(CHUNKS):
        first = c * size
        out, spans = chunk_products(
            raws[c], next_counts[:, first : first + size], standard, first, share, haplo_total
        )
        n = len(spans)
        sums = gather(out[:n], out[n:], spans, [0] * n, width + first, sums)
    rates = rates_of(share, width * genome)
    score, local, last = local_sums(ends, sums, place, rates, genome * samples)
    table = lax.all_to_all(last[:, None], ("genome", "samples"), 0, 0, tiled=True)[:, 0]
    log_rates = jnp.array(rates, jnp.float32)[:, None]
    position = (place[1] * share + jnp.arange(share, dtype=jnp.int32)).astype(jnp.float32) + 1.0
    norm = jnp.expm1(log_rates) / jnp.expm1(position[None] * log_rates)
    profile = finish(local, table, norm, place, rates)
    return score[0], profile


def solution(mesh):
    return jax.shard_map(
        per_device,
        mesh=mesh,
        in_specs=(P("samples", "genome"), P(("genome", "samples"))),
        out_specs=(P(("genome", "samples")), P(None, ("genome", "samples"))),
        check_vma=False,
    )
```

```python
import functools
import math

import jax
import jax.numpy as jnp
from jax import lax
from jax.experimental import pallas as pl
from jax.experimental.pallas import tpu as pltpu
from jax.sharding import PartitionSpec as P


LANES = 128
EIGHTHS = (2, 3, 2, 1)
VMEM_LIMIT = 20 * 2**20
variance_floor = 0.01


def standardize(alleles, frequency, inverse_sd):
    return ((alleles.astype(jnp.float32) - frequency) * inverse_sd).astype(jnp.bfloat16)


def product(left, right):
    return lax.dot_general(
        left, right, (((0,), (0,)), ((), ())), preferred_element_type=jnp.float32
    )


def moments(counts, haplo_total):
    frequency = counts / haplo_total
    return frequency, lax.rsqrt(jnp.maximum(frequency * (1.0 - frequency), variance_floor))


def call(kernel, shapes, *arrays):
    return pl.pallas_call(
        kernel,
        in_specs=[pl.BlockSpec(memory_space=pltpu.VMEM)] * len(arrays),
        out_specs=[pl.BlockSpec(memory_space=pltpu.VMEM)] * len(shapes),
        out_shape=[jax.ShapeDtypeStruct(s, t) for s, t in shapes],
        compiler_params=pltpu.CompilerParams(vmem_limit_bytes=VMEM_LIMIT),
    )(*arrays)


def columns(index, width):
    return pl.ds(pl.multiple_of(index * width, LANES), width)


def expm1(x):
    series = jnp.ones_like(x)
    for n in range(9, 1, -1):
        series = 1.0 + series * (x * (1.0 / n))
    return jnp.where(x > -0.35, x * series, jnp.exp(x) - 1.0)


def own_kernel(share, haplo_total, rates, hap_ref, counts_ref, std_ref, low_ref, high_ref, low_send, high_send, norm_ref, token_ref):
    token_ref[...] = jnp.zeros_like(token_ref)
    me = lax.axis_index("genome") * lax.axis_size("samples") + lax.axis_index("samples")
    position = (me * share + lax.broadcasted_iota(jnp.int32, (1, share), 1)).astype(jnp.float32) + 1.0
    for k, rate in enumerate(rates):
        norm_ref[k : k + 1, :] = math.expm1(rate) / expm1(position * rate)
    frequency, inverse_sd = moments(counts_ref[...], haplo_total)
    std_ref[...] = standardize(hap_ref[...], frequency, inverse_sd)
    mine = lax.axis_index("samples")
    other = 1 - mine
    later = std_ref[:, share:]
    high_send[...] = product(later, std_ref[:, columns(other, share)]).astype(jnp.bfloat16)
    low = product(std_ref[:, :share], std_ref[:, :share])
    low_ref[...] = low
    low_send[...] = low.astype(jnp.bfloat16)
    high_ref[...] = product(later, std_ref[:, columns(mine, share)])


def both_kernel(first, share, haplo_total, raw_ref, counts_ref, std_ref, before_ref, keep_ref, send_ref, token_ref):
    token_ref[...] = before_ref[...]
    frequency, inverse_sd = moments(counts_ref[:, first : first + raw_ref.shape[1]], haplo_total)
    later = standardize(raw_ref[...], frequency, inverse_sd)
    mine = lax.axis_index("samples")
    other = 1 - mine
    send_ref[...] = product(later, std_ref[:, columns(other, share)]).astype(jnp.bfloat16)
    keep_ref[...] = product(later, std_ref[:, columns(mine, share)])


def last_kernel(first, haplo_total, raw_ref, counts_ref, std_ref, before_ref, keep_ref, send_ref, token_ref):
    token_ref[...] = before_ref[...]
    frequency, inverse_sd = moments(counts_ref[:, first : first + raw_ref.shape[1]], haplo_total)
    later = standardize(raw_ref[...], frequency, inverse_sd)
    keep = product(later, std_ref[:, first:])
    keep_ref[...] = keep
    send_ref[...] = keep.astype(jnp.bfloat16)


def window_sums(total, haplo_total, first_column, first_row, ends):
    correlation = total / haplo_total
    column = first_column + lax.broadcasted_iota(jnp.int32, total.shape, 0)
    row = first_row + lax.broadcasted_iota(jnp.int32, total.shape, 1)
    inside = (column > row) & (column < ends)
    return jnp.sum(jnp.where(inside, correlation * correlation, 0.0), axis=0, keepdims=True)


def local_ends(ends_ref, share):
    start = lax.axis_index("genome") * (lax.axis_size("samples") * share)
    return ends_ref[...] - start


def early_kernel(share, haplo_total, pieces, ends_ref, *refs):
    out_ref = refs[-1]
    mine = lax.axis_index("samples")
    ends = local_ends(ends_ref, share)
    out_ref[...] = jnp.zeros_like(out_ref)
    for k, (first_column, owner) in enumerate(pieces):
        keep, got = refs[2 * k], refs[2 * k + 1]

        def add(keep=keep, got=got, first_column=first_column):
            total = keep[...] + got[...].astype(jnp.float32)
            out_ref[...] += window_sums(total, haplo_total, first_column, mine * share, ends)

        if owner is None:
            add()
        else:
            pl.when(mine == owner)(add)


def rates_of(share, variants):
    return (math.log(0.5) / (4 * share), math.log(0.1) / variants)


def tail_kernel(share, haplo_total, pieces, rates, ends_ref, sums_ref, *refs):
    n = len(pieces)
    score_ref, local_ref, last_ref, total_ref = refs[2 * n :]
    mine = lax.axis_index("samples")
    ends = local_ends(ends_ref, share)
    total_ref[...] = sums_ref[...]
    for k, (first_column, first_row, owner) in enumerate(pieces):
        keep, got = refs[2 * k], refs[2 * k + 1]

        @pl.when(mine == owner)
        def _(keep=keep, got=got, first_column=first_column, first_row=first_row, owner=owner):
            inner = slice(first_row - owner * share, None)
            total = keep[...] + got[...].astype(jnp.float32)
            total_ref[:, inner] += window_sums(
                total, haplo_total, first_column, first_row, ends[:, inner]
            )

    row = mine * share + lax.broadcasted_iota(jnp.int32, (1, share), 1)
    counted = jnp.maximum(ends - row - 1, 1).astype(jnp.float32)
    score = total_ref[...] / counted
    score_ref[...] = score
    blocks = share // LANES
    stacked = jnp.concatenate(
        [score[:, b * LANES : (b + 1) * LANES] for b in range(blocks)]
        + ([jnp.zeros(((-blocks) % 8, LANES), jnp.float32)] if blocks % 8 else []),
        axis=0,
    )
    source = lax.broadcasted_iota(jnp.int32, (LANES, LANES), 0)
    target = lax.broadcasted_iota(jnp.int32, (LANES, LANES), 1)
    lag = (target - source).astype(jnp.float32)
    lane = lax.broadcasted_iota(jnp.int32, (1, LANES), 1).astype(jnp.float32)
    lasts = []
    for k, rate in enumerate(rates):
        weight = jnp.where(lag >= 0.0, jnp.exp(jnp.maximum(lag, 0.0) * rate), 0.0)
        inner = lax.dot_general(
            stacked,
            weight,
            (((1,), (0,)), ((), ())),
            precision=lax.Precision.HIGHEST,
            preferred_element_type=jnp.float32,
        )
        fall = jnp.exp((lane + 1.0) * rate)
        carry = jnp.zeros((1, 1), jnp.float32)
        for b in range(blocks):
            here = inner[b : b + 1, :] + carry * fall
            local_ref[k : k + 1, b * LANES : (b + 1) * LANES] = here
            carry = here[:, LANES - 1 :]
        lasts.append(carry)
    tile_lane = lax.broadcasted_iota(jnp.int32, last_ref.shape, 1)
    last_ref[...] = jnp.where(tile_lane == 0, lasts[0], jnp.where(tile_lane == 1, lasts[1], 0.0))


def finish_kernel(rates, local_ref, table_ref, norm_ref, profile_ref):
    share = local_ref.shape[1]
    peers = table_ref.shape[0]
    me = lax.axis_index("genome") * lax.axis_size("samples") + lax.axis_index("samples")
    peer = lax.broadcasted_iota(jnp.int32, (peers, LANES), 0)
    gap = ((me - 1 - peer) * share).astype(jnp.float32)
    step = lax.broadcasted_iota(jnp.int32, (1, share), 1).astype(jnp.float32)
    for k, rate in enumerate(rates):
        weight = jnp.where(peer < me, jnp.exp(jnp.maximum(gap, 0.0) * rate), 0.0)
        incoming = jnp.sum(weight * table_ref[...], axis=0, keepdims=True)[:, k : k + 1]
        smoothed = local_ref[k : k + 1, :] + incoming * jnp.exp((step + 1.0) * rate)
        profile_ref[k : k + 1, :] = smoothed * norm_ref[k : k + 1, :]


def per_device(haplotypes, window_ends):
    samples = lax.axis_size("samples")
    genome = lax.axis_size("genome")
    depth, width = haplotypes.shape
    share = width // samples
    haplo_total = float(depth * samples)
    rates = rates_of(share, width * genome)
    back = [(i + 1, i) for i in range(genome - 1)]
    ends = window_ends[None]
    f32, bf16 = jnp.float32, jnp.bfloat16
    unit = width // 8
    firsts = [unit * sum(EIGHTHS[:c]) for c in range(len(EIGHTHS))]
    sizes = [unit * e for e in EIGHTHS]

    raws, counts = [], None
    for first, size in zip(firsts, sizes):
        raws.append(lax.ppermute(haplotypes[:, first : first + size], "genome", back))
    counts = jnp.sum(haplotypes, axis=0, dtype=f32)[None]
    if samples == 2:
        counts = counts + lax.ppermute(counts, "samples", [(0, 1), (1, 0)])
    else:
        counts = lax.psum(counts, "samples")
    next_counts = lax.ppermute(counts, "genome", back)

    def swap(send, pairs):
        return lax.ppermute(send, "samples", pairs)

    both, up, down = [(0, 1), (1, 0)], [(0, 1)], [(1, 0)]
    tails, tail_pieces = [], []
    token_type = ((8, LANES), f32)
    if samples == 2:
        standard, low, high, low_send, high_send, norm, token = call(
            functools.partial(own_kernel, share, haplo_total, rates),
            [((depth, width), bf16)]
            + [((share, share), f32)] * 2
            + [((share, share), bf16)] * 2
            + [((2, share), f32), token_type],
            haplotypes,
            counts,
        )
        arrays = [high, swap(high_send, both), low, swap(low_send, down)]
        pieces = [(share, None), (0, 0)]
        for c, (first, size) in enumerate(zip(firsts, sizes)):
            straddles = first < share
            rows = share if straddles else width - first
            kernel = (
                functools.partial(both_kernel, first, share, haplo_total)
                if straddles
                else functools.partial(last_kernel, first, haplo_total)
            )
            keep, send, token = call(
                kernel,
                [((size, rows), f32), ((size, rows), bf16), token_type],
                raws[c],
                next_counts,
                standard,
                token,
            )
            got = swap(send, both if straddles else up)
            if straddles:
                arrays += [keep, got]
                pieces.append((width + first, None))
            else:
                tails += [keep, got]
                tail_pieces.append((width + first, first, 1))
        (sums,) = call(
            functools.partial(early_kernel, share, haplo_total, pieces),
            [((1, share), f32)],
            ends,
            *arrays,
        )
    else:
        frequency, inverse_sd = moments(counts, haplo_total)
        standard = standardize(haplotypes, frequency, inverse_sd)
        frequency, inverse_sd = moments(next_counts, haplo_total)
        later = standardize(jnp.concatenate(raws, axis=1), frequency, inverse_sd)
        total = lax.psum_scatter(
            product(jnp.concatenate([standard, later], axis=1), standard),
            "samples",
            scatter_dimension=1,
            tiled=True,
        )
        me = lax.axis_index("genome") * samples + lax.axis_index("samples")
        position = (me * share + jnp.arange(share, dtype=jnp.int32)).astype(f32) + 1.0
        log_rates = jnp.array(rates, f32)[:, None]
        norm = jnp.expm1(log_rates) / jnp.expm1(position[None] * log_rates)
        sums = window_sums(
            total,
            haplo_total,
            0,
            lax.axis_index("samples") * share,
            ends - lax.axis_index("genome") * width,
        )

    score, local, last, _ = call(
        functools.partial(tail_kernel, share, haplo_total, tail_pieces, rates),
        [((1, share), f32), ((2, share), f32), ((genome * samples, LANES), f32), ((1, share), f32)],
        ends,
        sums,
        *tails,
    )
    table = lax.all_to_all(last[:, None], ("genome", "samples"), 0, 0, tiled=True)[:, 0]
    (profile,) = call(
        functools.partial(finish_kernel, rates), [((2, share), f32)], local, table, norm
    )
    return score[0], profile


def solution(mesh):
    return jax.shard_map(
        per_device,
        mesh=mesh,
        in_specs=(P("samples", "genome"), P(("genome", "samples"))),
        out_specs=(P(("genome", "samples")), P(None, ("genome", "samples"))),
        check_vma=False,
    )
```

```python
import functools
import math

import jax
import jax.numpy as jnp
from jax import lax
from jax.experimental import pallas as pl
from jax.experimental.pallas import tpu as pltpu
from jax.sharding import PartitionSpec as P


LANES = 128
EIGHTHS = (2, 3, 2, 1)
VMEM_LIMIT = 20 * 2**20
variance_floor = 0.01


def standardize(alleles, frequency, inverse_sd):
    return ((alleles.astype(jnp.float32) - frequency) * inverse_sd).astype(jnp.bfloat16)


def product(left, right):
    return lax.dot_general(
        left, right, (((0,), (0,)), ((), ())), preferred_element_type=jnp.float32
    )


def moments(counts, haplo_total):
    frequency = counts / haplo_total
    return frequency, lax.rsqrt(jnp.maximum(frequency * (1.0 - frequency), variance_floor))


def call(kernel, shapes, *arrays):
    return pl.pallas_call(
        kernel,
        in_specs=[pl.BlockSpec(memory_space=pltpu.VMEM)] * len(arrays),
        out_specs=[pl.BlockSpec(memory_space=pltpu.VMEM)] * len(shapes),
        out_shape=[jax.ShapeDtypeStruct(s, t) for s, t in shapes],
        compiler_params=pltpu.CompilerParams(vmem_limit_bytes=VMEM_LIMIT),
    )(*arrays)


def expm1(x):
    series = jnp.ones_like(x)
    for n in range(9, 1, -1):
        series = 1.0 + series * (x * (1.0 / n))
    return jnp.where(x > -0.35, x * series, jnp.exp(x) - 1.0)


def expm1(x):
    series = jnp.ones_like(x)
    for n in range(9, 1, -1):
        series = 1.0 + series * (x * (1.0 / n))
    return jnp.where(x > -0.35, x * series, jnp.exp(x) - 1.0)


def band_blocks(columns, rows, block):
    out = []
    for column in range(columns[0], columns[1], block):
        stop = min(columns[1], column + block)
        last = min(rows[1], stop)
        if out and out[-1][2] == rows[0] and last == rows[1] and out[-1][3] == rows[1] - rows[0]:
            first, count, row, length = out[-1]
            out[-1] = (first, count + stop - column, row, length)
        elif last > rows[0]:
            out.append((column, stop - column, rows[0], last - rows[0]))
    return out


def band_low(first, stop, share):
    return [(first, stop - first, first, share - first)]


def multiply_blocks(left_ref, left_first, right_ref, messages):
    mine = lax.axis_index("samples")
    for owner, blocks, keeps, sends in messages:
        for (column, count, row, length), keep, send in zip(blocks, keeps, sends):
            part = product(
                left_ref[:, column - left_first : column - left_first + count],
                right_ref[:, row : row + length],
            )

            @pl.when(mine == owner)
            def _(keep=keep, part=part):
                keep[...] = part

            @pl.when(mine != owner)
            def _(send=send, part=part):
                send[...] = part.astype(jnp.bfloat16)


def split_refs(groups, refs):
    messages, at = [], 0
    for owner, blocks in groups:
        n = len(blocks)
        messages.append((owner, blocks, refs[at : at + n], refs[at + n : at + 2 * n]))
        at += 2 * n
    return messages


def counts_kernel(hap_ref, out_ref):
    out_ref[...] = jnp.sum(hap_ref[...].astype(jnp.float32), axis=0, keepdims=True)


def own_kernel(groups, share, haplo_total, rates, hap_ref, counts_ref, std_ref, norm_ref, token_ref, *refs):
    token_ref[...] = jnp.zeros_like(token_ref)
    frequency, inverse_sd = moments(counts_ref[...], haplo_total)
    std_ref[...] = standardize(hap_ref[...], frequency, inverse_sd)
    multiply_blocks(std_ref, 0, std_ref, split_refs(groups, refs))
    me = lax.axis_index("genome") * lax.axis_size("samples") + lax.axis_index("samples")
    position = (me * share + lax.broadcasted_iota(jnp.int32, (1, share), 1)).astype(jnp.float32) + 1.0
    for k, rate in enumerate(rates):
        norm_ref[k : k + 1, :] = math.expm1(rate) / expm1(position * rate)


def chunk_kernel(groups, first, haplo_total, raw_ref, counts_ref, std_ref, before_ref, token_ref, later_ref, *refs):
    token_ref[...] = before_ref[...]
    frequency, inverse_sd = moments(counts_ref[:, first : first + raw_ref.shape[1]], haplo_total)
    later_ref[...] = standardize(raw_ref[...], frequency, inverse_sd)
    multiply_blocks(later_ref, first, std_ref, split_refs(groups, refs))


def window_sums(total, haplo_total, first_column, first_row, ends):
    correlation = total / haplo_total
    column = first_column + lax.broadcasted_iota(jnp.int32, total.shape, 0)
    row = first_row + lax.broadcasted_iota(jnp.int32, total.shape, 1)
    inside = (column > row) & (column < ends)
    return jnp.sum(jnp.where(inside, correlation * correlation, 0.0), axis=0, keepdims=True)


def local_ends(ends_ref, share):
    start = lax.axis_index("genome") * (lax.axis_size("samples") * share)
    return ends_ref[...] - start


def add_blocks(pieces, refs, share, haplo_total, ends, out_ref):
    mine = lax.axis_index("samples")
    for k, (owner, first_column, first_row) in enumerate(pieces):
        keep, got = refs[2 * k], refs[2 * k + 1]

        @pl.when(mine == owner)
        def _(keep=keep, got=got, owner=owner, first_column=first_column, first_row=first_row):
            start = first_row - owner * share
            inner = slice(start, start + keep.shape[1])
            total = keep[...] + got[...].astype(jnp.float32)
            out_ref[:, inner] += window_sums(total, haplo_total, first_column, first_row, ends[:, inner])


def early_kernel(share, haplo_total, pieces, ends_ref, *refs):
    out_ref = refs[-1]
    out_ref[...] = jnp.zeros_like(out_ref)
    add_blocks(pieces, refs, share, haplo_total, local_ends(ends_ref, share), out_ref)


def rates_of(share, variants):
    return (math.log(0.5) / (4 * share), math.log(0.1) / variants)


def tail_kernel(share, haplo_total, pieces, rates, ends_ref, sums_ref, *refs):
    n = len(pieces)
    score_ref, local_ref, last_ref, total_ref = refs[2 * n :]
    mine = lax.axis_index("samples")
    ends = local_ends(ends_ref, share)
    total_ref[...] = sums_ref[...]
    add_blocks(pieces, refs, share, haplo_total, ends, total_ref)
    row = mine * share + lax.broadcasted_iota(jnp.int32, (1, share), 1)
    counted = jnp.maximum(ends - row - 1, 1).astype(jnp.float32)
    score = total_ref[...] / counted
    score_ref[...] = score
    blocks = share // LANES
    stacked = jnp.concatenate(
        [score[:, b * LANES : (b + 1) * LANES] for b in range(blocks)]
        + ([jnp.zeros(((-blocks) % 8, LANES), jnp.float32)] if blocks % 8 else []),
        axis=0,
    )
    source = lax.broadcasted_iota(jnp.int32, (LANES, LANES), 0)
    target = lax.broadcasted_iota(jnp.int32, (LANES, LANES), 1)
    lag = (target - source).astype(jnp.float32)
    lane = lax.broadcasted_iota(jnp.int32, (1, LANES), 1).astype(jnp.float32)
    lasts = []
    for k, rate in enumerate(rates):
        weight = jnp.where(lag >= 0.0, jnp.exp(jnp.maximum(lag, 0.0) * rate), 0.0)
        inner = lax.dot_general(
            stacked,
            weight,
            (((1,), (0,)), ((), ())),
            precision=lax.Precision.HIGHEST,
            preferred_element_type=jnp.float32,
        )
        fall = jnp.exp((lane + 1.0) * rate)
        carry = jnp.zeros((1, 1), jnp.float32)
        for b in range(blocks):
            here = inner[b : b + 1, :] + carry * fall
            local_ref[k : k + 1, b * LANES : (b + 1) * LANES] = here
            carry = here[:, LANES - 1 :]
        lasts.append(carry)
    tile_lane = lax.broadcasted_iota(jnp.int32, last_ref.shape, 1)
    last_ref[...] = jnp.where(tile_lane == 0, lasts[0], jnp.where(tile_lane == 1, lasts[1], 0.0))


def finish_kernel(rates, local_ref, table_ref, norm_ref, profile_ref):
    share = local_ref.shape[1]
    peers = table_ref.shape[0]
    me = lax.axis_index("genome") * lax.axis_size("samples") + lax.axis_index("samples")
    peer = lax.broadcasted_iota(jnp.int32, (peers, LANES), 0)
    gap = ((me - 1 - peer) * share).astype(jnp.float32)
    step = lax.broadcasted_iota(jnp.int32, (1, share), 1).astype(jnp.float32)
    for k, rate in enumerate(rates):
        weight = jnp.where(peer < me, jnp.exp(jnp.maximum(gap, 0.0) * rate), 0.0)
        incoming = jnp.sum(weight * table_ref[...], axis=0, keepdims=True)[:, k : k + 1]
        smoothed = local_ref[k : k + 1, :] + incoming * jnp.exp((step + 1.0) * rate)
        profile_ref[k : k + 1, :] = smoothed * norm_ref[k : k + 1, :]


def per_device(haplotypes, window_ends):
    samples = lax.axis_size("samples")
    genome = lax.axis_size("genome")
    depth, width = haplotypes.shape
    share = width // samples
    haplo_total = float(depth * samples)
    rates = rates_of(share, width * genome)
    back = [(i + 1, i) for i in range(genome - 1)]
    ends = window_ends[None]
    f32, bf16 = jnp.float32, jnp.bfloat16
    unit = width // 8
    firsts = [unit * sum(EIGHTHS[:c]) for c in range(len(EIGHTHS))]
    sizes = [unit * e for e in EIGHTHS]

    def shifted(array, c):
        return lax.ppermute(array[:, firsts[c] : firsts[c] + sizes[c]], "genome", back)

    raws = [shifted(haplotypes, 0)]
    (counts,) = call(counts_kernel, [((1, width), f32)], haplotypes)
    behind, counts = lax.optimization_barrier((haplotypes, counts))
    raws += [shifted(behind, c) for c in range(1, len(EIGHTHS))]
    if samples == 2:
        counts = counts + lax.ppermute(counts, "samples", [(0, 1), (1, 0)])
    else:
        counts = lax.psum(counts, "samples")
    next_counts = lax.ppermute(counts, "genome", back)

    def swap(owner, sends):
        return [lax.ppermute(send, "samples", [(1 - owner, owner)]) for send in sends]

    def shapes_of(groups):
        shapes = []
        for _, blocks in groups:
            for kind in (f32, bf16):
                shapes += [((count, length), kind) for _, count, _, length in blocks]
        return shapes

    tails, tail_pieces = [], []
    token_type = ((8, LANES), f32)
    if samples == 2:
        block = share // 2
        groups = [
            (1, band_blocks((share, width), (share, width), block)),
            (0, [(share, width - share, 0, share)]),
            (0, band_blocks((0, share), (0, share), block)),
        ]
        standard, norm, token, *outs = call(
            functools.partial(own_kernel, groups, share, haplo_total, rates),
            [((depth, width), bf16), ((2, share), f32), token_type] + shapes_of(groups),
            haplotypes,
            counts,
        )
        arrays, pieces = [], []

        def exchange(groups, outs, shift):
            added, where = [], []
            for owner, blocks, keeps, sends in split_refs(groups, outs):
                for keep, got, (column, _, row, _) in zip(keeps, swap(owner, sends), blocks):
                    added += [keep, got]
                    where.append((owner, column + shift, row))
            return added, where

        added, where = exchange(groups, outs, 0)
        arrays += added
        pieces += where
        for c, (first, size) in enumerate(zip(firsts, sizes)):
            stop = first + size
            groups = [(1, [(first, size, max(first, share), width - max(first, share))])]
            if first < share:
                low = min(stop, share)
                groups.append((0, band_low(first, low, share)))
            token, _, *outs = call(
                functools.partial(chunk_kernel, groups, first, haplo_total),
                [token_type, ((depth, size), bf16)] + shapes_of(groups),
                raws[c],
                next_counts,
                standard,
                token,
            )
            added, where = exchange(groups, outs, width)
            if first < share:
                arrays += added
                pieces += where
            else:
                tails += added
                tail_pieces += where
        (sums,) = call(
            functools.partial(early_kernel, share, haplo_total, pieces),
            [((1, share), f32)],
            ends,
            *arrays,
        )
    else:
        frequency, inverse_sd = moments(counts, haplo_total)
        standard = standardize(haplotypes, frequency, inverse_sd)
        frequency, inverse_sd = moments(next_counts, haplo_total)
        later = standardize(jnp.concatenate(raws, axis=1), frequency, inverse_sd)
        total = lax.psum_scatter(
            product(jnp.concatenate([standard, later], axis=1), standard),
            "samples",
            scatter_dimension=1,
            tiled=True,
        )
        me = lax.axis_index("genome") * samples + lax.axis_index("samples")
        position = (me * share + jnp.arange(share, dtype=jnp.int32)).astype(f32) + 1.0
        log_rates = jnp.array(rates, f32)[:, None]
        norm = jnp.expm1(log_rates) / jnp.expm1(position[None] * log_rates)
        sums = window_sums(
            total,
            haplo_total,
            0,
            lax.axis_index("samples") * share,
            ends - lax.axis_index("genome") * width,
        )

    score, local, last, _ = call(
        functools.partial(tail_kernel, share, haplo_total, tail_pieces, rates),
        [((1, share), f32), ((2, share), f32), ((genome * samples, LANES), f32), ((1, share), f32)],
        ends,
        sums,
        *tails,
    )
    table = lax.all_to_all(last[:, None], ("genome", "samples"), 0, 0, tiled=True)[:, 0]
    (profile,) = call(
        functools.partial(finish_kernel, rates), [((2, share), f32)], local, table, norm
    )
    return score[0], profile


def solution(mesh):
    return jax.shard_map(
        per_device,
        mesh=mesh,
        in_specs=(P("samples", "genome"), P(("genome", "samples"))),
        out_specs=(P(("genome", "samples")), P(None, ("genome", "samples"))),
        check_vma=False,
    )
```

```python
import functools
import math

import jax
import jax.numpy as jnp
from jax import lax
from jax.experimental import pallas as pl
from jax.experimental.pallas import tpu as pltpu
from jax.sharding import PartitionSpec as P


LANES = 128
EIGHTHS = (1, 2, 2, 2, 1)
VMEM_LIMIT = 20 * 2**20
variance_floor = 0.01


def standardize(alleles, frequency, inverse_sd):
    return ((alleles.astype(jnp.float32) - frequency) * inverse_sd).astype(jnp.bfloat16)


def product(left, right):
    return lax.dot_general(
        left, right, (((0,), (0,)), ((), ())), preferred_element_type=jnp.float32
    )


def moments(counts, haplo_total):
    frequency = counts / haplo_total
    return frequency, lax.rsqrt(jnp.maximum(frequency * (1.0 - frequency), variance_floor))


def call(kernel, shapes, *arrays):
    return pl.pallas_call(
        kernel,
        in_specs=[pl.BlockSpec(memory_space=pltpu.VMEM)] * len(arrays),
        out_specs=[pl.BlockSpec(memory_space=pltpu.VMEM)] * len(shapes),
        out_shape=[jax.ShapeDtypeStruct(s, t) for s, t in shapes],
        compiler_params=pltpu.CompilerParams(vmem_limit_bytes=VMEM_LIMIT),
    )(*arrays)


def columns(index, width):
    return pl.ds(pl.multiple_of(index * width, LANES), width)


def expm1(x):
    series = jnp.ones_like(x)
    for n in range(9, 1, -1):
        series = 1.0 + series * (x * (1.0 / n))
    return jnp.where(x > -0.35, x * series, jnp.exp(x) - 1.0)


def load_kernel(hap_hbm, hap_ref, out_ref, arrived):
    parts = arrived.shape[0]
    rows = hap_ref.shape[0] // parts
    copies = [
        pltpu.make_async_copy(
            hap_hbm.at[pl.ds(k * rows, rows)], hap_ref.at[pl.ds(k * rows, rows)], arrived.at[k]
        )
        for k in range(parts)
    ]
    for copy in copies:
        copy.start()
    out_ref[...] = jnp.zeros_like(out_ref)
    for k, copy in enumerate(copies):
        copy.wait()
        block = hap_ref[k * rows : (k + 1) * rows, :].astype(jnp.float32)
        out_ref[...] += jnp.sum(block, axis=0, keepdims=True)


def load(haplotypes):
    return pl.pallas_call(
        load_kernel,
        in_specs=[pl.BlockSpec(memory_space=pl.ANY)],
        out_specs=[pl.BlockSpec(memory_space=pltpu.VMEM)] * 2,
        out_shape=[
            jax.ShapeDtypeStruct(haplotypes.shape, haplotypes.dtype),
            jax.ShapeDtypeStruct((1, haplotypes.shape[1]), jnp.float32),
        ],
        scratch_shapes=[pltpu.SemaphoreType.DMA((4,))],
        compiler_params=pltpu.CompilerParams(vmem_limit_bytes=VMEM_LIMIT),
        name="local_counts",
    )(haplotypes)


def standardize_part(raw_ref, counts_ref, first, haplo_total):
    frequency, inverse_sd = moments(counts_ref[:, first : first + raw_ref.shape[1]], haplo_total)
    return standardize(raw_ref[...], frequency, inverse_sd)


def own_kernel(
    share, haplo_total, rates, hap_ref, counts_ref,
    std_ref, norm_ref, token_ref, high_ref, send_ref, low_ref, low_send_1, low_send_2,
):
    token_ref[...] = jnp.zeros_like(token_ref)
    std_ref[...] = standardize_part(hap_ref, counts_ref, 0, haplo_total)
    mine = lax.axis_index("samples")
    half = share // 2
    later = std_ref[:, share:]
    send_ref[...] = product(later, std_ref[:, columns(1 - mine, share)]).astype(jnp.bfloat16)
    high_ref[...] = product(later, std_ref[:, columns(mine, share)])
    low = product(std_ref[:, half:share], std_ref[:, :share])
    low_ref[half:, :] = low
    low_send_1[...] = low.astype(jnp.bfloat16)
    low = product(std_ref[:, :half], std_ref[:, :half])
    low_ref[:half, :half] = low
    low_send_2[...] = low.astype(jnp.bfloat16)
    me = lax.axis_index("genome") * lax.axis_size("samples") + mine
    position = (me * share + lax.broadcasted_iota(jnp.int32, (1, share), 1)).astype(jnp.float32) + 1.0
    for k, rate in enumerate(rates):
        norm_ref[k : k + 1, :] = math.expm1(rate) / expm1(position * rate)


def first_kernel(
    share, haplo_total, raw_0, raw_1, counts_ref, std_ref, before_ref, token_ref, keep_ref, send_ref, later_ref
):
    token_ref[...] = before_ref[...]
    unit = raw_0.shape[1]
    later_ref[:, :unit] = standardize_part(raw_0, counts_ref, 0, haplo_total)
    later_ref[:, unit:] = standardize_part(raw_1, counts_ref, unit, haplo_total)
    mine = lax.axis_index("samples")
    send_ref[...] = product(later_ref[...], std_ref[:, columns(1 - mine, share)]).astype(jnp.bfloat16)
    keep_ref[...] = product(later_ref[...], std_ref[:, columns(mine, share)])


def middle_kernel(
    first, share, haplo_total, raw_ref, counts_ref, std_ref, low_send_1, before_ref,
    token_ref, keep_ref, send_ref, corner_ref, corner_send,
):
    token_ref[...] = before_ref[...]
    later = standardize_part(raw_ref, counts_ref, first, haplo_total)
    keep = product(later, std_ref[:, share:])
    keep_ref[...] = keep
    corner = product(later[:, : share - first], std_ref[:, first:share])
    corner_ref[...] = corner
    corner_send[...] = corner.astype(jnp.bfloat16)
    mine = lax.axis_index("samples")

    @pl.when(mine == 0)
    def _():
        send_ref[...] = keep.astype(jnp.bfloat16)

    @pl.when(mine == 1)
    def _():
        send_ref[...] = low_send_1[...]


def upper_kernel(
    first, haplo_total, raw_ref, counts_ref, std_ref, low_send_2, corner_send, before_ref,
    token_ref, keep_ref, send_ref,
):
    token_ref[...] = before_ref[...]
    later = standardize_part(raw_ref, counts_ref, first, haplo_total)
    keep = product(later, std_ref[:, first:])
    keep_ref[...] = keep
    mine = lax.axis_index("samples")

    @pl.when(mine == 0)
    def _():
        send_ref[...] = keep.astype(jnp.bfloat16)

    @pl.when(mine == 1)
    def _():
        half, corner = low_send_2.shape[1], corner_send.shape[0]
        send_ref[:, :half] = low_send_2[...]
        send_ref[:corner, half:] = corner_send[...]
        send_ref[corner:, half:] = jnp.zeros_like(send_ref[corner:, half:])


def last_kernel(first, haplo_total, raw_ref, counts_ref, std_ref, keep_ref, send_ref):
    later = standardize_part(raw_ref, counts_ref, first, haplo_total)
    keep = product(later, std_ref[:, first:])
    keep_ref[...] = keep
    send_ref[...] = keep.astype(jnp.bfloat16)


def window_sums(total, haplo_total, first_column, first_row, ends):
    correlation = total / haplo_total
    column = first_column + lax.broadcasted_iota(jnp.int32, total.shape, 0)
    row = first_row + lax.broadcasted_iota(jnp.int32, total.shape, 1)
    inside = (column > row) & (column < ends)
    return jnp.sum(jnp.where(inside, correlation * correlation, 0.0), axis=0, keepdims=True)


def local_ends(ends_ref, share):
    start = lax.axis_index("genome") * (lax.axis_size("samples") * share)
    return ends_ref[...] - start


def add_blocks(pieces, refs, share, haplo_total, ends, out_ref):
    mine = lax.axis_index("samples")
    for owner, keep, keep_at, got, got_at, first_column, first_row in pieces:

        def add(keep=keep, keep_at=keep_at, got=got, got_at=got_at, first_column=first_column, first_row=first_row):
            total = refs[keep][keep_at] + refs[got][got_at].astype(jnp.float32)
            start = first_row % share
            inner = slice(start, start + total.shape[1])
            row = mine * share + start
            out_ref[:, inner] += window_sums(total, haplo_total, first_column, row, ends[:, inner])

        if owner is None:
            add()
        else:
            pl.when(mine == owner)(add)


def early_kernel(share, haplo_total, pieces, ends_ref, *refs):
    out_ref = refs[-1]
    out_ref[...] = jnp.zeros_like(out_ref)
    add_blocks(pieces, refs, share, haplo_total, local_ends(ends_ref, share), out_ref)


def rates_of(share, variants):
    return (math.log(0.5) / (4 * share), math.log(0.1) / variants)


def tail_kernel(share, haplo_total, pieces, rates, ends_ref, sums_ref, *refs):
    score_ref, local_ref, last_ref, total_ref = refs[-4:]
    mine = lax.axis_index("samples")
    ends = local_ends(ends_ref, share)
    total_ref[...] = sums_ref[...]
    add_blocks(pieces, refs, share, haplo_total, ends, total_ref)
    row = mine * share + lax.broadcasted_iota(jnp.int32, (1, share), 1)
    counted = jnp.maximum(ends - row - 1, 1).astype(jnp.float32)
    score = total_ref[...] / counted
    score_ref[...] = score
    blocks = share // LANES
    stacked = jnp.concatenate(
        [score[:, b * LANES : (b + 1) * LANES] for b in range(blocks)]
        + ([jnp.zeros(((-blocks) % 8, LANES), jnp.float32)] if blocks % 8 else []),
        axis=0,
    )
    source = lax.broadcasted_iota(jnp.int32, (LANES, LANES), 0)
    target = lax.broadcasted_iota(jnp.int32, (LANES, LANES), 1)
    lag = (target - source).astype(jnp.float32)
    lane = lax.broadcasted_iota(jnp.int32, (1, LANES), 1).astype(jnp.float32)
    lasts = []
    for k, rate in enumerate(rates):
        weight = jnp.where(lag >= 0.0, jnp.exp(jnp.maximum(lag, 0.0) * rate), 0.0)
        inner = lax.dot_general(
            stacked,
            weight,
            (((1,), (0,)), ((), ())),
            precision=lax.Precision.HIGHEST,
            preferred_element_type=jnp.float32,
        )
        fall = jnp.exp((lane + 1.0) * rate)
        carry = jnp.zeros((1, 1), jnp.float32)
        for b in range(blocks):
            here = inner[b : b + 1, :] + carry * fall
            local_ref[k : k + 1, b * LANES : (b + 1) * LANES] = here
            carry = here[:, LANES - 1 :]
        lasts.append(carry)
    tile_lane = lax.broadcasted_iota(jnp.int32, last_ref.shape, 1)
    last_ref[...] = jnp.where(tile_lane == 0, lasts[0], jnp.where(tile_lane == 1, lasts[1], 0.0))


def finish_kernel(rates, local_ref, table_ref, norm_ref, profile_ref):
    share = local_ref.shape[1]
    peers = table_ref.shape[0]
    me = lax.axis_index("genome") * lax.axis_size("samples") + lax.axis_index("samples")
    peer = lax.broadcasted_iota(jnp.int32, (peers, LANES), 0)
    gap = ((me - 1 - peer) * share).astype(jnp.float32)
    step = lax.broadcasted_iota(jnp.int32, (1, share), 1).astype(jnp.float32)
    for k, rate in enumerate(rates):
        weight = jnp.where(peer < me, jnp.exp(jnp.maximum(gap, 0.0) * rate), 0.0)
        incoming = jnp.sum(weight * table_ref[...], axis=0, keepdims=True)[:, k : k + 1]
        smoothed = local_ref[k : k + 1, :] + incoming * jnp.exp((step + 1.0) * rate)
        profile_ref[k : k + 1, :] = smoothed * norm_ref[k : k + 1, :]


def per_device(haplotypes, window_ends):
    samples = lax.axis_size("samples")
    genome = lax.axis_size("genome")
    depth, width = haplotypes.shape
    share = width // samples
    haplo_total = float(depth * samples)
    rates = rates_of(share, width * genome)
    back = [(i + 1, i) for i in range(genome - 1)]
    ends = window_ends[None]
    f32, bf16 = jnp.float32, jnp.bfloat16
    unit = width // 8
    firsts = [unit * sum(EIGHTHS[:c]) for c in range(len(EIGHTHS))]
    sizes = [unit * e for e in EIGHTHS]

    def shifted(array, c):
        return lax.ppermute(array[:, firsts[c] : firsts[c] + sizes[c]], "genome", back)

    raws = [shifted(haplotypes, 0)]
    haplotypes, counts = load(haplotypes)
    raws += [shifted(haplotypes, c) for c in range(1, len(EIGHTHS))]
    if samples == 2:
        counts = counts + lax.ppermute(counts, "samples", [(0, 1), (1, 0)])
    else:
        counts = lax.psum(counts, "samples")
    next_counts = lax.ppermute(counts, "genome", back)

    def swap(send, pairs=((0, 1), (1, 0))):
        return lax.ppermute(send, "samples", pairs)

    tails, tail_pieces = [], []
    token_type = ((8, LANES), f32)
    if samples == 2:
        half, u, whole = share // 2, unit, slice(None)
        standard, norm, token, high, send, low, low_send_1, low_send_2 = call(
            functools.partial(own_kernel, share, haplo_total, rates),
            [((depth, width), bf16), ((2, share), f32), token_type]
            + [((share, share), f32), ((share, share), bf16), ((share, share), f32)]
            + [((half, share), bf16), ((half, half), bf16)],
            haplotypes,
            counts,
        )
        got_0 = swap(send)
        token, keep_1, send, _ = call(
            functools.partial(first_kernel, share, haplo_total),
            [token_type, ((3 * u, share), f32), ((3 * u, share), bf16), ((depth, 3 * u), bf16)],
            raws[0],
            raws[1],
            next_counts,
            standard,
            token,
        )
        got_1 = swap(send)
        token, keep_2, send, corner, corner_send = call(
            functools.partial(middle_kernel, firsts[2], share, haplo_total),
            [token_type, ((2 * u, share), f32), ((2 * u, share), bf16), ((u, u), f32), ((u, u), bf16)],
            raws[2],
            next_counts,
            standard,
            low_send_1,
            token,
        )
        got_2 = swap(send)
        token, keep_3, send = call(
            functools.partial(upper_kernel, firsts[3], haplo_total),
            [token_type, ((2 * u, 3 * u), f32), ((2 * u, 3 * u), bf16)],
            raws[3],
            next_counts,
            standard,
            low_send_2,
            corner_send,
            token,
        )
        got_3 = swap(send)
        pieces = [
            (None, 0, (whole, whole), 1, (whole, whole), share, 0),
            (None, 2, (whole, whole), 3, (whole, whole), width, 0),
            (0, 4, (slice(half, None), whole), 6, (whole, whole), half, 0),
            (1, 5, (whole, whole), 6, (whole, whole), width + firsts[2], share),
        ]
        (sums,) = call(
            functools.partial(early_kernel, share, haplo_total, pieces),
            [((1, share), f32)],
            ends,
            high,
            got_0,
            keep_1,
            got_1,
            low,
            keep_2,
            got_2,
        )
        keep_4, send = call(
            functools.partial(last_kernel, firsts[4], haplo_total),
            [((u, u), f32), ((u, u), bf16)],
            raws[4],
            next_counts,
            standard,
        )
        got_4 = swap(send, [(0, 1)])
        tails = [low, corner, keep_3, got_3, keep_4, got_4]
        tail_pieces = [
            (0, 0, (slice(0, half), slice(0, half)), 3, (whole, slice(0, half)), 0, 0),
            (0, 1, (whole, whole), 3, (slice(0, u), slice(half, None)), width + firsts[2], firsts[2]),
            (1, 2, (whole, whole), 3, (whole, whole), width + firsts[3], firsts[3]),
            (1, 4, (whole, whole), 5, (whole, whole), width + firsts[4], firsts[4]),
        ]
    else:
        frequency, inverse_sd = moments(counts, haplo_total)
        standard = standardize(haplotypes, frequency, inverse_sd)
        frequency, inverse_sd = moments(next_counts, haplo_total)
        later = standardize(jnp.concatenate(raws, axis=1), frequency, inverse_sd)
        total = lax.psum_scatter(
            product(jnp.concatenate([standard, later], axis=1), standard),
            "samples",
            scatter_dimension=1,
            tiled=True,
        )
        me = lax.axis_index("genome") * samples + lax.axis_index("samples")
        position = (me * share + jnp.arange(share, dtype=jnp.int32)).astype(f32) + 1.0
        log_rates = jnp.array(rates, f32)[:, None]
        norm = jnp.expm1(log_rates) / jnp.expm1(position[None] * log_rates)
        sums = window_sums(
            total,
            haplo_total,
            0,
            lax.axis_index("samples") * share,
            ends - lax.axis_index("genome") * width,
        )

    score, local, last, _ = call(
        functools.partial(tail_kernel, share, haplo_total, tail_pieces, rates),
        [((1, share), f32), ((2, share), f32), ((genome * samples, LANES), f32), ((1, share), f32)],
        ends,
        sums,
        *tails,
    )
    table = lax.all_to_all(last[:, None], ("genome", "samples"), 0, 0, tiled=True)[:, 0]
    (profile,) = call(
        functools.partial(finish_kernel, rates), [((2, share), f32)], local, table, norm
    )
    return score[0], profile


def solution(mesh):
    return jax.shard_map(
        per_device,
        mesh=mesh,
        in_specs=(P("samples", "genome"), P(("genome", "samples"))),
        out_specs=(P(("genome", "samples")), P(None, ("genome", "samples"))),
        check_vma=False,
    )
```

```python
import functools
import math

import jax
import jax.numpy as jnp
from jax import lax
from jax.experimental import pallas as pl
from jax.experimental.pallas import tpu as pltpu
from jax.sharding import PartitionSpec as P


LANES = 128
EIGHTHS = (2, 2, 2, 1, 1)
VMEM_LIMIT = 20 * 2**20
variance_floor = 0.01


def standardize(alleles, frequency, inverse_sd):
    return ((alleles.astype(jnp.float32) - frequency) * inverse_sd).astype(jnp.bfloat16)


def product(left, right):
    return lax.dot_general(
        left, right, (((0,), (0,)), ((), ())), preferred_element_type=jnp.float32
    )


def moments(counts, haplo_total):
    frequency = counts / haplo_total
    return frequency, lax.rsqrt(jnp.maximum(frequency * (1.0 - frequency), variance_floor))


def call(kernel, shapes, *arrays):
    return pl.pallas_call(
        kernel,
        in_specs=[pl.BlockSpec(memory_space=pltpu.VMEM)] * len(arrays),
        out_specs=[pl.BlockSpec(memory_space=pltpu.VMEM)] * len(shapes),
        out_shape=[jax.ShapeDtypeStruct(s, t) for s, t in shapes],
        compiler_params=pltpu.CompilerParams(vmem_limit_bytes=VMEM_LIMIT),
    )(*arrays)


def columns(index, width):
    return pl.ds(pl.multiple_of(index * width, LANES), width)


def expm1(x):
    series = jnp.ones_like(x)
    for n in range(9, 1, -1):
        series = 1.0 + series * (x * (1.0 / n))
    return jnp.where(x > -0.35, x * series, jnp.exp(x) - 1.0)


def load_kernel(hap_hbm, hap_ref, out_ref, arrived):
    parts = arrived.shape[0]
    rows = hap_ref.shape[0] // parts
    copies = [
        pltpu.make_async_copy(
            hap_hbm.at[pl.ds(k * rows, rows)], hap_ref.at[pl.ds(k * rows, rows)], arrived.at[k]
        )
        for k in range(parts)
    ]
    for copy in copies:
        copy.start()
    out_ref[...] = jnp.zeros_like(out_ref)
    for k, copy in enumerate(copies):
        copy.wait()
        block = hap_ref[k * rows : (k + 1) * rows, :].astype(jnp.float32)
        out_ref[...] += jnp.sum(block, axis=0, keepdims=True)


def load(haplotypes):
    return pl.pallas_call(
        load_kernel,
        in_specs=[pl.BlockSpec(memory_space=pltpu.HBM)],
        out_specs=[pl.BlockSpec(memory_space=pltpu.VMEM)] * 2,
        out_shape=[
            jax.ShapeDtypeStruct(haplotypes.shape, haplotypes.dtype),
            jax.ShapeDtypeStruct((1, haplotypes.shape[1]), jnp.float32),
        ],
        scratch_shapes=[pltpu.SemaphoreType.DMA((4,))],
        compiler_params=pltpu.CompilerParams(vmem_limit_bytes=VMEM_LIMIT),
        name="local_counts",
    )(pltpu.with_memory_space_constraint(haplotypes, pltpu.HBM))


def standardize_part(raw_ref, counts_ref, first, haplo_total):
    frequency, inverse_sd = moments(counts_ref[:, first : first + raw_ref.shape[1]], haplo_total)
    return standardize(raw_ref[...], frequency, inverse_sd)


def own_kernel(
    share, haplo_total, rates, hap_ref, counts_ref,
    std_ref, norm_ref, token_ref, high_ref, send_ref, low_ref, low_send_1, low_send_2,
):
    token_ref[...] = jnp.zeros_like(token_ref)
    std_ref[...] = standardize_part(hap_ref, counts_ref, 0, haplo_total)
    mine = lax.axis_index("samples")
    half = share // 2
    later = std_ref[:, share:]
    send_ref[...] = product(later, std_ref[:, columns(1 - mine, share)]).astype(jnp.bfloat16)
    high_ref[...] = product(later, std_ref[:, columns(mine, share)])
    low = product(std_ref[:, half:share], std_ref[:, :share])
    low_ref[half:, :] = low
    low_send_1[...] = low.astype(jnp.bfloat16)
    low = product(std_ref[:, :half], std_ref[:, :half])
    low_ref[:half, :half] = low
    low_send_2[...] = low.astype(jnp.bfloat16)
    me = lax.axis_index("genome") * lax.axis_size("samples") + mine
    position = (me * share + lax.broadcasted_iota(jnp.int32, (1, share), 1)).astype(jnp.float32) + 1.0
    for k, rate in enumerate(rates):
        norm_ref[k : k + 1, :] = math.expm1(rate) / expm1(position * rate)


def first_kernel(
    share, haplo_total, raw_0, raw_1, counts_ref, std_ref, low_send_2, before_ref,
    token_ref, keep_ref, send_ref, later_ref,
):
    token_ref[...] = before_ref[...]
    half = raw_0.shape[1]
    later_ref[:, :half] = standardize_part(raw_0, counts_ref, 0, haplo_total)
    later_ref[:, half:] = standardize_part(raw_1, counts_ref, half, haplo_total)
    mine = lax.axis_index("samples")
    send_ref[...] = product(later_ref[...], std_ref[:, columns(1 - mine, share)]).astype(jnp.bfloat16)

    @pl.when(mine == 1)
    def _():
        send_ref[half:, :half] = low_send_2[...]

    keep_ref[...] = product(later_ref[...], std_ref[:, columns(mine, share)])


def middle_kernel(
    first, share, haplo_total, raw_ref, counts_ref, std_ref, low_send_1, before_ref,
    token_ref, keep_ref, send_ref,
):
    token_ref[...] = before_ref[...]
    later = standardize_part(raw_ref, counts_ref, first, haplo_total)
    keep = product(later, std_ref[:, share:])
    keep_ref[...] = keep
    mine = lax.axis_index("samples")

    @pl.when(mine == 0)
    def _():
        send_ref[...] = keep.astype(jnp.bfloat16)

    @pl.when(mine == 1)
    def _():
        send_ref[...] = low_send_1[...]


def upper_kernel(
    first, haplo_total, raw_ref, counts_ref, std_ref, before_ref, token_ref, keep_ref, send_ref
):
    token_ref[...] = before_ref[...]
    later = standardize_part(raw_ref, counts_ref, first, haplo_total)
    keep = product(later, std_ref[:, first:])
    keep_ref[...] = keep
    send_ref[...] = keep.astype(jnp.bfloat16)


def window_sums(total, haplo_total, first_column, first_row, ends):
    correlation = total / haplo_total
    column = first_column + lax.broadcasted_iota(jnp.int32, total.shape, 0)
    row = first_row + lax.broadcasted_iota(jnp.int32, total.shape, 1)
    inside = (column > row) & (column < ends)
    return jnp.sum(jnp.where(inside, correlation * correlation, 0.0), axis=0, keepdims=True)


def local_ends(ends_ref, share):
    start = lax.axis_index("genome") * (lax.axis_size("samples") * share)
    return ends_ref[...] - start


def add_blocks(pieces, refs, share, haplo_total, ends, out_ref):
    mine = lax.axis_index("samples")
    for owner, keep, keep_at, got, got_at, first_column, first_row in pieces:

        def add(keep=keep, keep_at=keep_at, got=got, got_at=got_at, first_column=first_column, first_row=first_row):
            total = refs[keep][keep_at] + refs[got][got_at].astype(jnp.float32)
            start = first_row % share
            inner = slice(start, start + total.shape[1])
            row = mine * share + start
            out_ref[:, inner] += window_sums(total, haplo_total, first_column, row, ends[:, inner])

        if owner is None:
            add()
        else:
            pl.when(mine == owner)(add)


def early_kernel(share, haplo_total, pieces, ends_ref, *refs):
    out_ref = refs[-1]
    out_ref[...] = jnp.zeros_like(out_ref)
    add_blocks(pieces, refs, share, haplo_total, local_ends(ends_ref, share), out_ref)


def rates_of(share, variants):
    return (math.log(0.5) / (4 * share), math.log(0.1) / variants)


def tail_kernel(share, haplo_total, pieces, rates, ends_ref, sums_ref, *refs):
    score_ref, local_ref, last_ref, total_ref = refs[-4:]
    mine = lax.axis_index("samples")
    ends = local_ends(ends_ref, share)
    total_ref[...] = sums_ref[...]
    add_blocks(pieces, refs, share, haplo_total, ends, total_ref)
    row = mine * share + lax.broadcasted_iota(jnp.int32, (1, share), 1)
    counted = jnp.maximum(ends - row - 1, 1).astype(jnp.float32)
    score = total_ref[...] / counted
    score_ref[...] = score
    blocks = share // LANES
    stacked = jnp.concatenate(
        [score[:, b * LANES : (b + 1) * LANES] for b in range(blocks)]
        + ([jnp.zeros(((-blocks) % 8, LANES), jnp.float32)] if blocks % 8 else []),
        axis=0,
    )
    source = lax.broadcasted_iota(jnp.int32, (LANES, LANES), 0)
    target = lax.broadcasted_iota(jnp.int32, (LANES, LANES), 1)
    lag = (target - source).astype(jnp.float32)
    lane = lax.broadcasted_iota(jnp.int32, (1, LANES), 1).astype(jnp.float32)
    lasts = []
    for k, rate in enumerate(rates):
        weight = jnp.where(lag >= 0.0, jnp.exp(jnp.maximum(lag, 0.0) * rate), 0.0)
        inner = lax.dot_general(
            stacked,
            weight,
            (((1,), (0,)), ((), ())),
            precision=lax.Precision.HIGHEST,
            preferred_element_type=jnp.float32,
        )
        fall = jnp.exp((lane + 1.0) * rate)
        carry = jnp.zeros((1, 1), jnp.float32)
        for b in range(blocks):
            here = inner[b : b + 1, :] + carry * fall
            local_ref[k : k + 1, b * LANES : (b + 1) * LANES] = here
            carry = here[:, LANES - 1 :]
        lasts.append(carry)
    tile_lane = lax.broadcasted_iota(jnp.int32, last_ref.shape, 1)
    last_ref[...] = jnp.where(tile_lane == 0, lasts[0], jnp.where(tile_lane == 1, lasts[1], 0.0))


def finish_kernel(rates, local_ref, table_ref, norm_ref, profile_ref):
    share = local_ref.shape[1]
    peers = table_ref.shape[0]
    me = lax.axis_index("genome") * lax.axis_size("samples") + lax.axis_index("samples")
    peer = lax.broadcasted_iota(jnp.int32, (peers, LANES), 0)
    gap = ((me - 1 - peer) * share).astype(jnp.float32)
    step = lax.broadcasted_iota(jnp.int32, (1, share), 1).astype(jnp.float32)
    for k, rate in enumerate(rates):
        weight = jnp.where(peer < me, jnp.exp(jnp.maximum(gap, 0.0) * rate), 0.0)
        incoming = jnp.sum(weight * table_ref[...], axis=0, keepdims=True)[:, k : k + 1]
        smoothed = local_ref[k : k + 1, :] + incoming * jnp.exp((step + 1.0) * rate)
        profile_ref[k : k + 1, :] = smoothed * norm_ref[k : k + 1, :]


def per_device(haplotypes, window_ends):
    samples = lax.axis_size("samples")
    genome = lax.axis_size("genome")
    depth, width = haplotypes.shape
    share = width // samples
    haplo_total = float(depth * samples)
    rates = rates_of(share, width * genome)
    back = [(i + 1, i) for i in range(genome - 1)]
    ends = window_ends[None]
    f32, bf16 = jnp.float32, jnp.bfloat16
    unit = width // 8
    firsts = [unit * sum(EIGHTHS[:c]) for c in range(len(EIGHTHS))]
    sizes = [unit * e for e in EIGHTHS]

    def shifted(array, c):
        return lax.ppermute(array[:, firsts[c] : firsts[c] + sizes[c]], "genome", back)

    raws = [shifted(haplotypes, 0)]
    haplotypes, counts = load(haplotypes)
    raws += [shifted(haplotypes, c) for c in range(1, len(EIGHTHS))]
    if samples == 2:
        counts = counts + lax.ppermute(counts, "samples", [(0, 1), (1, 0)])
    else:
        counts = lax.psum(counts, "samples")
    next_counts = lax.ppermute(counts, "genome", back)

    def swap(send, pairs=((0, 1), (1, 0))):
        return lax.ppermute(send, "samples", pairs)

    tails, tail_pieces = [], []
    token_type = ((8, LANES), f32)
    if samples == 2:
        half, whole = share // 2, slice(None)
        standard, norm, token, high, send, low, low_send_1, low_send_2 = call(
            functools.partial(own_kernel, share, haplo_total, rates),
            [((depth, width), bf16), ((2, share), f32), token_type]
            + [((share, share), f32), ((share, share), bf16), ((share, share), f32)]
            + [((half, share), bf16), ((half, half), bf16)],
            haplotypes,
            counts,
        )
        got_0 = swap(send)
        token, keep_1, send, _ = call(
            functools.partial(first_kernel, share, haplo_total),
            [token_type, ((share, share), f32), ((share, share), bf16), ((depth, share), bf16)],
            raws[0],
            raws[1],
            next_counts,
            standard,
            low_send_2,
            token,
        )
        got_1 = swap(send)
        token, keep_2, send = call(
            functools.partial(middle_kernel, firsts[2], share, haplo_total),
            [token_type, ((half, share), f32), ((half, share), bf16)],
            raws[2],
            next_counts,
            standard,
            low_send_1,
            token,
        )
        got_2 = swap(send)
        tails = []
        for c in (3, 4):
            shape = (sizes[c], width - firsts[c])
            token, keep, send = call(
                functools.partial(upper_kernel, firsts[c], haplo_total),
                [token_type, (shape, f32), (shape, bf16)],
                raws[c],
                next_counts,
                standard,
                token,
            )
            tails += [keep, swap(send, [(0, 1)])]
        lower, upper = slice(0, half), slice(half, None)
        pieces = [
            (None, 0, (whole, whole), 1, (whole, whole), share, 0),
            (0, 2, (lower, whole), 3, (lower, whole), width, 0),
            (0, 2, (upper, upper), 3, (upper, upper), width + half, half),
            (1, 2, (whole, whole), 3, (whole, whole), width, share),
            (0, 4, (lower, lower), 3, (upper, lower), 0, 0),
            (0, 4, (upper, whole), 6, (whole, whole), half, 0),
            (1, 5, (whole, whole), 6, (whole, whole), width + share, share),
        ]
        (sums,) = call(
            functools.partial(early_kernel, share, haplo_total, pieces),
            [((1, share), f32)],
            ends,
            high,
            got_0,
            keep_1,
            got_1,
            low,
            keep_2,
            got_2,
        )
        tail_pieces = [
            (1, 2 * k, (whole, whole), 2 * k + 1, (whole, whole), width + firsts[c], firsts[c])
            for k, c in enumerate((3, 4))
        ]
    else:
        frequency, inverse_sd = moments(counts, haplo_total)
        standard = standardize(haplotypes, frequency, inverse_sd)
        frequency, inverse_sd = moments(next_counts, haplo_total)
        later = standardize(jnp.concatenate(raws, axis=1), frequency, inverse_sd)
        total = lax.psum_scatter(
            product(jnp.concatenate([standard, later], axis=1), standard),
            "samples",
            scatter_dimension=1,
            tiled=True,
        )
        me = lax.axis_index("genome") * samples + lax.axis_index("samples")
        position = (me * share + jnp.arange(share, dtype=jnp.int32)).astype(f32) + 1.0
        log_rates = jnp.array(rates, f32)[:, None]
        norm = jnp.expm1(log_rates) / jnp.expm1(position[None] * log_rates)
        sums = window_sums(
            total,
            haplo_total,
            0,
            lax.axis_index("samples") * share,
            ends - lax.axis_index("genome") * width,
        )

    score, local, last, _ = call(
        functools.partial(tail_kernel, share, haplo_total, tail_pieces, rates),
        [((1, share), f32), ((2, share), f32), ((genome * samples, LANES), f32), ((1, share), f32)],
        ends,
        sums,
        *tails,
    )
    table = lax.all_to_all(last[:, None], ("genome", "samples"), 0, 0, tiled=True)[:, 0]
    (profile,) = call(
        functools.partial(finish_kernel, rates), [((2, share), f32)], local, table, norm
    )
    return score[0], profile


def solution(mesh):
    return jax.shard_map(
        per_device,
        mesh=mesh,
        in_specs=(P("samples", "genome"), P(("genome", "samples"))),
        out_specs=(P(("genome", "samples")), P(None, ("genome", "samples"))),
        check_vma=False,
    )
```

```python
import functools
import math

import jax
import jax.numpy as jnp
from jax import lax
from jax.experimental import pallas as pl
from jax.experimental.pallas import tpu as pltpu
from jax.sharding import PartitionSpec as P


LANES = 128
EIGHTHS = (3, 2, 2, 1)
VMEM_LIMIT = 20 * 2**20
variance_floor = 0.01


def standardize(alleles, frequency, inverse_sd):
    return ((alleles.astype(jnp.float32) - frequency) * inverse_sd).astype(jnp.bfloat16)


def product(left, right):
    return lax.dot_general(
        left, right, (((0,), (0,)), ((), ())), preferred_element_type=jnp.float32
    )


def moments(counts, haplo_total):
    frequency = counts / haplo_total
    return frequency, lax.rsqrt(jnp.maximum(frequency * (1.0 - frequency), variance_floor))


def call(kernel, shapes, *arrays):
    return pl.pallas_call(
        kernel,
        in_specs=[pl.BlockSpec(memory_space=pltpu.VMEM)] * len(arrays),
        out_specs=[pl.BlockSpec(memory_space=pltpu.VMEM)] * len(shapes),
        out_shape=[jax.ShapeDtypeStruct(s, t) for s, t in shapes],
        compiler_params=pltpu.CompilerParams(vmem_limit_bytes=VMEM_LIMIT),
    )(*arrays)


def columns(index, width):
    return pl.ds(pl.multiple_of(index * width, LANES), width)


def expm1(x):
    series = jnp.ones_like(x)
    for n in range(9, 1, -1):
        series = 1.0 + series * (x * (1.0 / n))
    return jnp.where(x > -0.35, x * series, jnp.exp(x) - 1.0)


def load_kernel(hap_hbm, hap_ref, out_ref, arrived):
    parts = arrived.shape[0]
    rows = hap_ref.shape[0] // parts
    copies = [
        pltpu.make_async_copy(
            hap_hbm.at[pl.ds(k * rows, rows)], hap_ref.at[pl.ds(k * rows, rows)], arrived.at[k]
        )
        for k in range(parts)
    ]
    for copy in copies:
        copy.start()
    out_ref[...] = jnp.zeros_like(out_ref)
    for k, copy in enumerate(copies):
        copy.wait()
        block = hap_ref[k * rows : (k + 1) * rows, :].astype(jnp.float32)
        out_ref[...] += jnp.sum(block, axis=0, keepdims=True)


def load(haplotypes):
    return pl.pallas_call(
        load_kernel,
        in_specs=[pl.BlockSpec(memory_space=pltpu.HBM)],
        out_specs=[pl.BlockSpec(memory_space=pltpu.VMEM)] * 2,
        out_shape=[
            jax.ShapeDtypeStruct(haplotypes.shape, haplotypes.dtype),
            jax.ShapeDtypeStruct((1, haplotypes.shape[1]), jnp.float32),
        ],
        scratch_shapes=[pltpu.SemaphoreType.DMA((4,))],
        compiler_params=pltpu.CompilerParams(vmem_limit_bytes=VMEM_LIMIT),
        name="local_counts",
    )(pltpu.with_memory_space_constraint(haplotypes, pltpu.HBM))


def standardize_part(raw_ref, counts_ref, first, haplo_total):
    frequency, inverse_sd = moments(counts_ref[:, first : first + raw_ref.shape[1]], haplo_total)
    return standardize(raw_ref[...], frequency, inverse_sd)


def own_kernel(
    share, haplo_total, rates, hap_ref, counts_ref,
    std_ref, norm_ref, token_ref, high_ref, send_ref, low_ref, low_send_1, low_send_2,
):
    token_ref[...] = jnp.zeros_like(token_ref)
    std_ref[...] = standardize_part(hap_ref, counts_ref, 0, haplo_total)
    mine = lax.axis_index("samples")
    half = share // 2
    later = std_ref[:, share:]
    send_ref[...] = product(later, std_ref[:, columns(1 - mine, share)]).astype(jnp.bfloat16)
    high_ref[...] = product(later, std_ref[:, columns(mine, share)])
    low = product(std_ref[:, half:share], std_ref[:, :share])
    low_ref[half:, :] = low
    low_send_1[...] = low.astype(jnp.bfloat16)
    low = product(std_ref[:, :half], std_ref[:, :half])
    low_ref[:half, :half] = low
    low_send_2[...] = low.astype(jnp.bfloat16)
    me = lax.axis_index("genome") * lax.axis_size("samples") + mine
    position = (me * share + lax.broadcasted_iota(jnp.int32, (1, share), 1)).astype(jnp.float32) + 1.0
    for k, rate in enumerate(rates):
        norm_ref[k : k + 1, :] = math.expm1(rate) / expm1(position * rate)


def first_kernel(
    share, haplo_total, raw_ref, counts_ref, std_ref, before_ref, token_ref, keep_ref, send_ref
):
    token_ref[...] = before_ref[...]
    later = standardize_part(raw_ref, counts_ref, 0, haplo_total)
    mine = lax.axis_index("samples")
    send_ref[...] = product(later, std_ref[:, columns(1 - mine, share)]).astype(jnp.bfloat16)
    keep_ref[...] = product(later, std_ref[:, columns(mine, share)])


def middle_kernel(
    first, share, haplo_total, raw_ref, counts_ref, std_ref, low_send_1, before_ref,
    token_ref, keep_ref, send_ref, corner_ref, corner_send,
):
    token_ref[...] = before_ref[...]
    later = standardize_part(raw_ref, counts_ref, first, haplo_total)
    keep = product(later, std_ref[:, share:])
    keep_ref[...] = keep
    corner = product(later[:, : share - first], std_ref[:, first:share])
    corner_ref[...] = corner
    corner_send[...] = corner.astype(jnp.bfloat16)
    mine = lax.axis_index("samples")

    @pl.when(mine == 0)
    def _():
        send_ref[...] = keep.astype(jnp.bfloat16)

    @pl.when(mine == 1)
    def _():
        send_ref[...] = low_send_1[...]


def upper_kernel(
    first, haplo_total, raw_ref, counts_ref, std_ref, low_send_2, corner_send, before_ref,
    token_ref, keep_ref, send_ref,
):
    token_ref[...] = before_ref[...]
    later = standardize_part(raw_ref, counts_ref, first, haplo_total)
    keep = product(later, std_ref[:, first:])
    keep_ref[...] = keep
    mine = lax.axis_index("samples")

    @pl.when(mine == 0)
    def _():
        send_ref[...] = keep.astype(jnp.bfloat16)

    @pl.when(mine == 1)
    def _():
        half, corner = low_send_2.shape[1], corner_send.shape[0]
        send_ref[:, :half] = low_send_2[...]
        send_ref[:corner, half:] = corner_send[...]
        send_ref[corner:, half:] = jnp.zeros_like(send_ref[corner:, half:])


def last_kernel(first, haplo_total, raw_ref, counts_ref, std_ref, keep_ref, send_ref):
    later = standardize_part(raw_ref, counts_ref, first, haplo_total)
    keep = product(later, std_ref[:, first:])
    keep_ref[...] = keep
    send_ref[...] = keep.astype(jnp.bfloat16)


def window_sums(total, haplo_total, first_column, first_row, ends):
    correlation = total / haplo_total
    column = first_column + lax.broadcasted_iota(jnp.int32, total.shape, 0)
    row = first_row + lax.broadcasted_iota(jnp.int32, total.shape, 1)
    inside = (column > row) & (column < ends)
    return jnp.sum(jnp.where(inside, correlation * correlation, 0.0), axis=0, keepdims=True)


def local_ends(ends_ref, share):
    start = lax.axis_index("genome") * (lax.axis_size("samples") * share)
    return ends_ref[...] - start


def add_blocks(pieces, refs, share, haplo_total, ends, out_ref):
    mine = lax.axis_index("samples")
    for owner, keep, keep_at, got, got_at, first_column, first_row in pieces:

        def add(keep=keep, keep_at=keep_at, got=got, got_at=got_at, first_column=first_column, first_row=first_row):
            total = refs[keep][keep_at] + refs[got][got_at].astype(jnp.float32)
            start = first_row % share
            inner = slice(start, start + total.shape[1])
            row = mine * share + start
            out_ref[:, inner] += window_sums(total, haplo_total, first_column, row, ends[:, inner])

        if owner is None:
            add()
        else:
            pl.when(mine == owner)(add)


def early_kernel(share, haplo_total, pieces, ends_ref, *refs):
    out_ref = refs[-1]
    out_ref[...] = jnp.zeros_like(out_ref)
    add_blocks(pieces, refs, share, haplo_total, local_ends(ends_ref, share), out_ref)


def rates_of(share, variants):
    return (math.log(0.5) / (4 * share), math.log(0.1) / variants)


def tail_kernel(share, haplo_total, pieces, rates, ends_ref, sums_ref, *refs):
    score_ref, local_ref, last_ref, total_ref = refs[-4:]
    mine = lax.axis_index("samples")
    ends = local_ends(ends_ref, share)
    total_ref[...] = sums_ref[...]
    add_blocks(pieces, refs, share, haplo_total, ends, total_ref)
    row = mine * share + lax.broadcasted_iota(jnp.int32, (1, share), 1)
    counted = jnp.maximum(ends - row - 1, 1).astype(jnp.float32)
    score = total_ref[...] / counted
    score_ref[...] = score
    blocks = share // LANES
    stacked = jnp.concatenate(
        [score[:, b * LANES : (b + 1) * LANES] for b in range(blocks)]
        + ([jnp.zeros(((-blocks) % 8, LANES), jnp.float32)] if blocks % 8 else []),
        axis=0,
    )
    source = lax.broadcasted_iota(jnp.int32, (LANES, LANES), 0)
    target = lax.broadcasted_iota(jnp.int32, (LANES, LANES), 1)
    lag = (target - source).astype(jnp.float32)
    lane = lax.broadcasted_iota(jnp.int32, (1, LANES), 1).astype(jnp.float32)
    lasts = []
    for k, rate in enumerate(rates):
        weight = jnp.where(lag >= 0.0, jnp.exp(jnp.maximum(lag, 0.0) * rate), 0.0)
        inner = lax.dot_general(
            stacked,
            weight,
            (((1,), (0,)), ((), ())),
            precision=lax.Precision.HIGHEST,
            preferred_element_type=jnp.float32,
        )
        fall = jnp.exp((lane + 1.0) * rate)
        carry = jnp.zeros((1, 1), jnp.float32)
        for b in range(blocks):
            here = inner[b : b + 1, :] + carry * fall
            local_ref[k : k + 1, b * LANES : (b + 1) * LANES] = here
            carry = here[:, LANES - 1 :]
        lasts.append(carry)
    tile_lane = lax.broadcasted_iota(jnp.int32, last_ref.shape, 1)
    last_ref[...] = jnp.where(tile_lane == 0, lasts[0], jnp.where(tile_lane == 1, lasts[1], 0.0))


def finish_kernel(rates, local_ref, table_ref, norm_ref, profile_ref):
    share = local_ref.shape[1]
    peers = table_ref.shape[0]
    me = lax.axis_index("genome") * lax.axis_size("samples") + lax.axis_index("samples")
    peer = lax.broadcasted_iota(jnp.int32, (peers, LANES), 0)
    gap = ((me - 1 - peer) * share).astype(jnp.float32)
    step = lax.broadcasted_iota(jnp.int32, (1, share), 1).astype(jnp.float32)
    for k, rate in enumerate(rates):
        weight = jnp.where(peer < me, jnp.exp(jnp.maximum(gap, 0.0) * rate), 0.0)
        incoming = jnp.sum(weight * table_ref[...], axis=0, keepdims=True)[:, k : k + 1]
        smoothed = local_ref[k : k + 1, :] + incoming * jnp.exp((step + 1.0) * rate)
        profile_ref[k : k + 1, :] = smoothed * norm_ref[k : k + 1, :]


def per_device(haplotypes, window_ends):
    samples = lax.axis_size("samples")
    genome = lax.axis_size("genome")
    depth, width = haplotypes.shape
    share = width // samples
    haplo_total = float(depth * samples)
    rates = rates_of(share, width * genome)
    back = [(i + 1, i) for i in range(genome - 1)]
    ends = window_ends[None]
    f32, bf16 = jnp.float32, jnp.bfloat16
    unit = width // 8
    firsts = [unit * sum(EIGHTHS[:c]) for c in range(len(EIGHTHS))]
    sizes = [unit * e for e in EIGHTHS]

    def shifted(array, c):
        return lax.ppermute(array[:, firsts[c] : firsts[c] + sizes[c]], "genome", back)

    raws = [shifted(haplotypes, 0)]
    haplotypes, counts = load(haplotypes)
    raws += [shifted(haplotypes, c) for c in range(1, len(EIGHTHS))]
    if samples == 2:
        counts = counts + lax.ppermute(counts, "samples", [(0, 1), (1, 0)])
    else:
        counts = lax.psum(counts, "samples")
    next_counts = lax.ppermute(counts, "genome", back)

    def swap(send, pairs=((0, 1), (1, 0))):
        return lax.ppermute(send, "samples", pairs)

    tails, tail_pieces = [], []
    token_type = ((8, LANES), f32)
    if samples == 2:
        half, u, whole = share // 2, unit, slice(None)
        standard, norm, token, high, send, low, low_send_1, low_send_2 = call(
            functools.partial(own_kernel, share, haplo_total, rates),
            [((depth, width), bf16), ((2, share), f32), token_type]
            + [((share, share), f32), ((share, share), bf16), ((share, share), f32)]
            + [((half, share), bf16), ((half, half), bf16)],
            haplotypes,
            counts,
        )
        got_0 = swap(send)
        token, keep_1, send = call(
            functools.partial(first_kernel, share, haplo_total),
            [token_type, ((3 * u, share), f32), ((3 * u, share), bf16)],
            raws[0],
            next_counts,
            standard,
            token,
        )
        got_1 = swap(send)
        token, keep_2, send, corner, corner_send = call(
            functools.partial(middle_kernel, firsts[1], share, haplo_total),
            [token_type, ((2 * u, share), f32), ((2 * u, share), bf16), ((u, u), f32), ((u, u), bf16)],
            raws[1],
            next_counts,
            standard,
            low_send_1,
            token,
        )
        got_2 = swap(send)
        token, keep_3, send = call(
            functools.partial(upper_kernel, firsts[2], haplo_total),
            [token_type, ((2 * u, 3 * u), f32), ((2 * u, 3 * u), bf16)],
            raws[2],
            next_counts,
            standard,
            low_send_2,
            corner_send,
            token,
        )
        got_3 = swap(send)
        pieces = [
            (None, 0, (whole, whole), 1, (whole, whole), share, 0),
            (None, 2, (whole, whole), 3, (whole, whole), width, 0),
            (0, 4, (slice(half, None), whole), 6, (whole, whole), half, 0),
            (1, 5, (whole, whole), 6, (whole, whole), width + firsts[1], share),
        ]
        (sums,) = call(
            functools.partial(early_kernel, share, haplo_total, pieces),
            [((1, share), f32)],
            ends,
            high,
            got_0,
            keep_1,
            got_1,
            low,
            keep_2,
            got_2,
        )
        keep_4, send = call(
            functools.partial(last_kernel, firsts[3], haplo_total),
            [((u, u), f32), ((u, u), bf16)],
            raws[3],
            next_counts,
            standard,
        )
        got_4 = swap(send, [(0, 1)])
        tails = [low, corner, keep_3, got_3, keep_4, got_4]
        tail_pieces = [
            (0, 0, (slice(0, half), slice(0, half)), 3, (whole, slice(0, half)), 0, 0),
            (0, 1, (whole, whole), 3, (slice(0, u), slice(half, None)), width + firsts[1], firsts[1]),
            (1, 2, (whole, whole), 3, (whole, whole), width + firsts[2], firsts[2]),
            (1, 4, (whole, whole), 5, (whole, whole), width + firsts[3], firsts[3]),
        ]
    else:
        frequency, inverse_sd = moments(counts, haplo_total)
        standard = standardize(haplotypes, frequency, inverse_sd)
        frequency, inverse_sd = moments(next_counts, haplo_total)
        later = standardize(jnp.concatenate(raws, axis=1), frequency, inverse_sd)
        total = lax.psum_scatter(
            product(jnp.concatenate([standard, later], axis=1), standard),
            "samples",
            scatter_dimension=1,
            tiled=True,
        )
        me = lax.axis_index("genome") * samples + lax.axis_index("samples")
        position = (me * share + jnp.arange(share, dtype=jnp.int32)).astype(f32) + 1.0
        log_rates = jnp.array(rates, f32)[:, None]
        norm = jnp.expm1(log_rates) / jnp.expm1(position[None] * log_rates)
        sums = window_sums(
            total,
            haplo_total,
            0,
            lax.axis_index("samples") * share,
            ends - lax.axis_index("genome") * width,
        )

    score, local, last, _ = call(
        functools.partial(tail_kernel, share, haplo_total, tail_pieces, rates),
        [((1, share), f32), ((2, share), f32), ((genome * samples, LANES), f32), ((1, share), f32)],
        ends,
        sums,
        *tails,
    )
    table = lax.all_to_all(last[:, None], ("genome", "samples"), 0, 0, tiled=True)[:, 0]
    (profile,) = call(
        functools.partial(finish_kernel, rates), [((2, share), f32)], local, table, norm
    )
    return score[0], profile


def solution(mesh):
    return jax.shard_map(
        per_device,
        mesh=mesh,
        in_specs=(P("samples", "genome"), P(("genome", "samples"))),
        out_specs=(P(("genome", "samples")), P(None, ("genome", "samples"))),
        check_vma=False,
    )
```

```python
import functools
import math

import jax
import jax.numpy as jnp
from jax import lax
from jax.experimental import pallas as pl
from jax.experimental.pallas import tpu as pltpu
from jax.sharding import PartitionSpec as P


LANES = 128
EIGHTHS = (3, 2, 1, 1, 1)
VMEM_LIMIT = 20 * 2**20
variance_floor = 0.01


def standardize(alleles, frequency, inverse_sd):
    return ((alleles.astype(jnp.float32) - frequency) * inverse_sd).astype(jnp.bfloat16)


def product(left, right):
    return lax.dot_general(
        left, right, (((0,), (0,)), ((), ())), preferred_element_type=jnp.float32
    )


def moments(counts, haplo_total):
    frequency = counts / haplo_total
    return frequency, lax.rsqrt(jnp.maximum(frequency * (1.0 - frequency), variance_floor))


def call(kernel, shapes, *arrays):
    return pl.pallas_call(
        kernel,
        in_specs=[pl.BlockSpec(memory_space=pltpu.VMEM)] * len(arrays),
        out_specs=[pl.BlockSpec(memory_space=pltpu.VMEM)] * len(shapes),
        out_shape=[jax.ShapeDtypeStruct(s, t) for s, t in shapes],
        compiler_params=pltpu.CompilerParams(vmem_limit_bytes=VMEM_LIMIT),
    )(*arrays)


def columns(index, width):
    return pl.ds(pl.multiple_of(index * width, LANES), width)


def expm1(x):
    series = jnp.ones_like(x)
    for n in range(9, 1, -1):
        series = 1.0 + series * (x * (1.0 / n))
    return jnp.where(x > -0.35, x * series, jnp.exp(x) - 1.0)


def load_kernel(hap_hbm, hap_ref, out_ref, arrived):
    parts = arrived.shape[0]
    rows = hap_ref.shape[0] // parts
    copies = [
        pltpu.make_async_copy(
            hap_hbm.at[pl.ds(k * rows, rows)], hap_ref.at[pl.ds(k * rows, rows)], arrived.at[k]
        )
        for k in range(parts)
    ]
    for copy in copies:
        copy.start()
    out_ref[...] = jnp.zeros_like(out_ref)
    for k, copy in enumerate(copies):
        copy.wait()
        block = hap_ref[k * rows : (k + 1) * rows, :].astype(jnp.float32)
        out_ref[...] += jnp.sum(block, axis=0, keepdims=True)


def load(haplotypes):
    return pl.pallas_call(
        load_kernel,
        in_specs=[pl.BlockSpec(memory_space=pltpu.HBM)],
        out_specs=[pl.BlockSpec(memory_space=pltpu.VMEM)] * 2,
        out_shape=[
            jax.ShapeDtypeStruct(haplotypes.shape, haplotypes.dtype),
            jax.ShapeDtypeStruct((1, haplotypes.shape[1]), jnp.float32),
        ],
        scratch_shapes=[pltpu.SemaphoreType.DMA((4,))],
        compiler_params=pltpu.CompilerParams(vmem_limit_bytes=VMEM_LIMIT),
        name="local_counts",
    )(pltpu.with_memory_space_constraint(haplotypes, pltpu.HBM))


def standardize_part(raw_ref, counts_ref, first, haplo_total):
    frequency, inverse_sd = moments(counts_ref[:, first : first + raw_ref.shape[1]], haplo_total)
    return standardize(raw_ref[...], frequency, inverse_sd)


def own_kernel(
    share, haplo_total, rates, hap_ref, counts_ref,
    std_ref, norm_ref, token_ref, high_ref, send_ref, low_ref, low_send_1, low_send_2,
):
    token_ref[...] = jnp.zeros_like(token_ref)
    std_ref[...] = standardize_part(hap_ref, counts_ref, 0, haplo_total)
    mine = lax.axis_index("samples")
    half = share // 2
    later = std_ref[:, share:]
    send_ref[...] = product(later, std_ref[:, columns(1 - mine, share)]).astype(jnp.bfloat16)
    high_ref[...] = product(later, std_ref[:, columns(mine, share)])
    low = product(std_ref[:, half:share], std_ref[:, :share])
    low_ref[half:, :] = low
    low_send_1[...] = low.astype(jnp.bfloat16)
    low = product(std_ref[:, :half], std_ref[:, :half])
    low_ref[:half, :half] = low
    low_send_2[...] = low.astype(jnp.bfloat16)
    me = lax.axis_index("genome") * lax.axis_size("samples") + mine
    position = (me * share + lax.broadcasted_iota(jnp.int32, (1, share), 1)).astype(jnp.float32) + 1.0
    for k, rate in enumerate(rates):
        norm_ref[k : k + 1, :] = math.expm1(rate) / expm1(position * rate)


def first_kernel(
    share, haplo_total, raw_ref, counts_ref, std_ref, before_ref, token_ref, keep_ref, send_ref
):
    token_ref[...] = before_ref[...]
    later = standardize_part(raw_ref, counts_ref, 0, haplo_total)
    mine = lax.axis_index("samples")
    send_ref[...] = product(later, std_ref[:, columns(1 - mine, share)]).astype(jnp.bfloat16)
    keep_ref[...] = product(later, std_ref[:, columns(mine, share)])


def middle_kernel(
    first, share, haplo_total, raw_ref, counts_ref, std_ref, low_send_1, before_ref,
    token_ref, keep_ref, send_ref, corner_ref, corner_send,
):
    token_ref[...] = before_ref[...]
    later = standardize_part(raw_ref, counts_ref, first, haplo_total)
    keep = product(later, std_ref[:, share:])
    keep_ref[...] = keep
    corner = product(later[:, : share - first], std_ref[:, first:share])
    corner_ref[...] = corner
    corner_send[...] = corner.astype(jnp.bfloat16)
    mine = lax.axis_index("samples")

    @pl.when(mine == 0)
    def _():
        send_ref[...] = keep.astype(jnp.bfloat16)

    @pl.when(mine == 1)
    def _():
        send_ref[...] = low_send_1[...]


def upper_kernel(first, haplo_total, fills, raw_ref, counts_ref, std_ref, before_ref, *refs):
    token_ref, keep_ref, send_ref = refs[len(fills) :]
    token_ref[...] = before_ref[...]
    later = standardize_part(raw_ref, counts_ref, first, haplo_total)
    keep = product(later, std_ref[:, first:])
    keep_ref[...] = keep
    mine = lax.axis_index("samples")

    @pl.when(mine == 0)
    def _():
        send_ref[...] = keep.astype(jnp.bfloat16)

    @pl.when(mine == 1)
    def _():
        for ref, rows, at in zip(refs, *zip(*fills)):
            send_ref[:, at] = ref[rows, :]


def last_kernel(first, haplo_total, raw_ref, counts_ref, std_ref, keep_ref, send_ref):
    later = standardize_part(raw_ref, counts_ref, first, haplo_total)
    keep = product(later, std_ref[:, first:])
    keep_ref[...] = keep
    send_ref[...] = keep.astype(jnp.bfloat16)


def window_sums(total, haplo_total, first_column, first_row, ends):
    correlation = total / haplo_total
    column = first_column + lax.broadcasted_iota(jnp.int32, total.shape, 0)
    row = first_row + lax.broadcasted_iota(jnp.int32, total.shape, 1)
    inside = (column > row) & (column < ends)
    return jnp.sum(jnp.where(inside, correlation * correlation, 0.0), axis=0, keepdims=True)


def local_ends(ends_ref, share):
    start = lax.axis_index("genome") * (lax.axis_size("samples") * share)
    return ends_ref[...] - start


def add_blocks(pieces, refs, share, haplo_total, ends, out_ref):
    mine = lax.axis_index("samples")
    for owner, keep, keep_at, got, got_at, first_column, first_row in pieces:

        def add(keep=keep, keep_at=keep_at, got=got, got_at=got_at, first_column=first_column, first_row=first_row):
            total = refs[keep][keep_at] + refs[got][got_at].astype(jnp.float32)
            start = first_row % share
            inner = slice(start, start + total.shape[1])
            row = mine * share + start
            out_ref[:, inner] += window_sums(total, haplo_total, first_column, row, ends[:, inner])

        if owner is None:
            add()
        else:
            pl.when(mine == owner)(add)


def early_kernel(share, haplo_total, pieces, ends_ref, *refs):
    out_ref = refs[-1]
    out_ref[...] = jnp.zeros_like(out_ref)
    add_blocks(pieces, refs, share, haplo_total, local_ends(ends_ref, share), out_ref)


def rates_of(share, variants):
    return (math.log(0.5) / (4 * share), math.log(0.1) / variants)


def tail_kernel(share, haplo_total, pieces, rates, ends_ref, sums_ref, *refs):
    score_ref, local_ref, last_ref, total_ref = refs[-4:]
    mine = lax.axis_index("samples")
    ends = local_ends(ends_ref, share)
    total_ref[...] = sums_ref[...]
    add_blocks(pieces, refs, share, haplo_total, ends, total_ref)
    row = mine * share + lax.broadcasted_iota(jnp.int32, (1, share), 1)
    counted = jnp.maximum(ends - row - 1, 1).astype(jnp.float32)
    score = total_ref[...] / counted
    score_ref[...] = score
    blocks = share // LANES
    stacked = jnp.concatenate(
        [score[:, b * LANES : (b + 1) * LANES] for b in range(blocks)]
        + ([jnp.zeros(((-blocks) % 8, LANES), jnp.float32)] if blocks % 8 else []),
        axis=0,
    )
    source = lax.broadcasted_iota(jnp.int32, (LANES, LANES), 0)
    target = lax.broadcasted_iota(jnp.int32, (LANES, LANES), 1)
    lag = (target - source).astype(jnp.float32)
    lane = lax.broadcasted_iota(jnp.int32, (1, LANES), 1).astype(jnp.float32)
    lasts = []
    for k, rate in enumerate(rates):
        weight = jnp.where(lag >= 0.0, jnp.exp(jnp.maximum(lag, 0.0) * rate), 0.0)
        to_end = jnp.exp((LANES - 1.0 - source.astype(jnp.float32)) * rate)
        inner, ending = (
            lax.dot_general(
                stacked,
                w,
                (((1,), (0,)), ((), ())),
                precision=lax.Precision.HIGHEST,
                preferred_element_type=jnp.float32,
            )
            for w in (weight, to_end)
        )
        fall = jnp.exp((lane + 1.0) * rate)
        block_fall = math.exp(LANES * rate)
        carry = jnp.zeros((1, LANES), jnp.float32)
        for b in range(blocks):
            local_ref[k : k + 1, b * LANES : (b + 1) * LANES] = inner[b : b + 1, :] + carry * fall
            carry = ending[b : b + 1, :] + carry * block_fall
        lasts.append(carry)
    tile_lane = lax.broadcasted_iota(jnp.int32, last_ref.shape, 1)
    last_ref[...] = jnp.where(tile_lane == 0, lasts[0], jnp.where(tile_lane == 1, lasts[1], 0.0))


def finish_kernel(rates, local_ref, table_ref, norm_ref, profile_ref):
    share = local_ref.shape[1]
    peers = table_ref.shape[0]
    me = lax.axis_index("genome") * lax.axis_size("samples") + lax.axis_index("samples")
    peer = lax.broadcasted_iota(jnp.int32, (peers, LANES), 0)
    gap = ((me - 1 - peer) * share).astype(jnp.float32)
    step = lax.broadcasted_iota(jnp.int32, (1, share), 1).astype(jnp.float32)
    for k, rate in enumerate(rates):
        weight = jnp.where(peer < me, jnp.exp(jnp.maximum(gap, 0.0) * rate), 0.0)
        incoming = jnp.sum(weight * table_ref[...], axis=0, keepdims=True)[:, k : k + 1]
        smoothed = local_ref[k : k + 1, :] + incoming * jnp.exp((step + 1.0) * rate)
        profile_ref[k : k + 1, :] = smoothed * norm_ref[k : k + 1, :]


def per_device(haplotypes, window_ends):
    samples = lax.axis_size("samples")
    genome = lax.axis_size("genome")
    depth, width = haplotypes.shape
    share = width // samples
    haplo_total = float(depth * samples)
    rates = rates_of(share, width * genome)
    back = [(i + 1, i) for i in range(genome - 1)]
    ends = window_ends[None]
    f32, bf16 = jnp.float32, jnp.bfloat16
    unit = width // 8
    firsts = [unit * sum(EIGHTHS[:c]) for c in range(len(EIGHTHS))]
    sizes = [unit * e for e in EIGHTHS]

    def shifted(array, c):
        return lax.ppermute(array[:, firsts[c] : firsts[c] + sizes[c]], "genome", back)

    raws = [shifted(haplotypes, 0)]
    haplotypes, counts = load(haplotypes)
    raws += [shifted(haplotypes, c) for c in range(1, len(EIGHTHS))]
    if samples == 2:
        counts = counts + lax.ppermute(counts, "samples", [(0, 1), (1, 0)])
    else:
        counts = lax.psum(counts, "samples")
    next_counts = lax.ppermute(counts, "genome", back)

    def swap(send, pairs=((0, 1), (1, 0))):
        return lax.ppermute(send, "samples", pairs)

    tails, tail_pieces = [], []
    token_type = ((8, LANES), f32)
    if samples == 2:
        half, u, whole = share // 2, unit, slice(None)
        standard, norm, token, high, send, low, low_send_1, low_send_2 = call(
            functools.partial(own_kernel, share, haplo_total, rates),
            [((depth, width), bf16), ((2, share), f32), token_type]
            + [((share, share), f32), ((share, share), bf16), ((share, share), f32)]
            + [((half, share), bf16), ((half, half), bf16)],
            haplotypes,
            counts,
        )
        got_0 = swap(send)
        token, keep_1, send = call(
            functools.partial(first_kernel, share, haplo_total),
            [token_type, ((3 * u, share), f32), ((3 * u, share), bf16)],
            raws[0],
            next_counts,
            standard,
            token,
        )
        got_1 = swap(send)
        token, keep_2, send, corner, corner_send = call(
            functools.partial(middle_kernel, firsts[1], share, haplo_total),
            [token_type, ((2 * u, share), f32), ((2 * u, share), bf16), ((u, u), f32), ((u, u), bf16)],
            raws[1],
            next_counts,
            standard,
            low_send_1,
            token,
        )
        got_2 = swap(send)
        first_unit, second_unit = slice(0, u), slice(u, None)
        lower, upper = slice(0, half), slice(half, None)
        tails = [low, corner]
        for c, fills, extra in (
            (2, [(first_unit, lower), (whole, upper)], [low_send_2, corner_send]),
            (3, [(second_unit, lower)], [low_send_2]),
        ):
            shape = (u, width - firsts[c])
            token, keep, send = call(
                functools.partial(upper_kernel, firsts[c], haplo_total, fills),
                [token_type, (shape, f32), (shape, bf16)],
                raws[c],
                next_counts,
                standard,
                token,
                *extra,
            )
            tails += [keep, swap(send)]
        pieces = [
            (None, 0, (whole, whole), 1, (whole, whole), share, 0),
            (None, 2, (whole, whole), 3, (whole, whole), width, 0),
            (0, 4, (slice(half, None), whole), 6, (whole, whole), half, 0),
            (1, 5, (whole, whole), 6, (whole, whole), width + firsts[1], share),
        ]
        (sums,) = call(
            functools.partial(early_kernel, share, haplo_total, pieces),
            [((1, share), f32)],
            ends,
            high,
            got_0,
            keep_1,
            got_1,
            low,
            keep_2,
            got_2,
        )
        keep, send = call(
            functools.partial(last_kernel, firsts[4], haplo_total),
            [((u, u), f32), ((u, u), bf16)],
            raws[4],
            next_counts,
            standard,
        )
        tails += [keep, swap(send, [(0, 1)])]
        tail_pieces = [
            (0, 0, (first_unit, lower), 3, (whole, lower), 0, 0),
            (0, 0, (slice(u, half), lower), 5, (whole, lower), u, 0),
            (0, 1, (whole, whole), 3, (whole, upper), width + firsts[1], firsts[1]),
        ] + [
            (1, 2 * c - 2, (whole, whole), 2 * c - 1, (whole, whole), width + firsts[c], firsts[c])
            for c in (2, 3, 4)
        ]
    else:
        frequency, inverse_sd = moments(counts, haplo_total)
        standard = standardize(haplotypes, frequency, inverse_sd)
        frequency, inverse_sd = moments(next_counts, haplo_total)
        later = standardize(jnp.concatenate(raws, axis=1), frequency, inverse_sd)
        total = lax.psum_scatter(
            product(jnp.concatenate([standard, later], axis=1), standard),
            "samples",
            scatter_dimension=1,
            tiled=True,
        )
        me = lax.axis_index("genome") * samples + lax.axis_index("samples")
        position = (me * share + jnp.arange(share, dtype=jnp.int32)).astype(f32) + 1.0
        log_rates = jnp.array(rates, f32)[:, None]
        norm = jnp.expm1(log_rates) / jnp.expm1(position[None] * log_rates)
        sums = window_sums(
            total,
            haplo_total,
            0,
            lax.axis_index("samples") * share,
            ends - lax.axis_index("genome") * width,
        )

    score, local, last, _ = call(
        functools.partial(tail_kernel, share, haplo_total, tail_pieces, rates),
        [((1, share), f32), ((2, share), f32), ((genome * samples, LANES), f32), ((1, share), f32)],
        ends,
        sums,
        *tails,
    )
    table = lax.all_to_all(last[:, None], ("genome", "samples"), 0, 0, tiled=True)[:, 0]
    (profile,) = call(
        functools.partial(finish_kernel, rates), [((2, share), f32)], local, table, norm
    )
    return score[0], profile


def solution(mesh):
    return jax.shard_map(
        per_device,
        mesh=mesh,
        in_specs=(P("samples", "genome"), P(("genome", "samples"))),
        out_specs=(P(("genome", "samples")), P(None, ("genome", "samples"))),
        check_vma=False,
    )
```

```python
import functools
import math

import jax
import jax.numpy as jnp
from jax import lax
from jax.experimental import pallas as pl
from jax.experimental.pallas import tpu as pltpu
from jax.sharding import PartitionSpec as P


LANES = 128
EIGHTHS = (3, 2, 1, 1, 1)
VMEM_LIMIT = 20 * 2**20
variance_floor = 0.01


def standardize(alleles, frequency, inverse_sd):
    return ((alleles.astype(jnp.float32) - frequency) * inverse_sd).astype(jnp.bfloat16)


def product(left, right):
    return lax.dot_general(
        left, right, (((0,), (0,)), ((), ())), preferred_element_type=jnp.float32
    )


def moments(counts, haplo_total):
    frequency = counts / haplo_total
    return frequency, lax.rsqrt(jnp.maximum(frequency * (1.0 - frequency), variance_floor))


def call(kernel, shapes, *arrays):
    return pl.pallas_call(
        kernel,
        in_specs=[pl.BlockSpec(memory_space=pltpu.VMEM)] * len(arrays),
        out_specs=[pl.BlockSpec(memory_space=pltpu.VMEM)] * len(shapes),
        out_shape=[jax.ShapeDtypeStruct(s, t) for s, t in shapes],
        compiler_params=pltpu.CompilerParams(vmem_limit_bytes=VMEM_LIMIT),
    )(*arrays)


def columns(index, width):
    return pl.ds(pl.multiple_of(index * width, LANES), width)


def expm1(x):
    series = jnp.ones_like(x)
    for n in range(9, 1, -1):
        series = 1.0 + series * (x * (1.0 / n))
    return jnp.where(x > -0.35, x * series, jnp.exp(x) - 1.0)


def load_kernel(hap_hbm, hap_ref, out_ref, arrived):
    parts = arrived.shape[0]
    rows = hap_ref.shape[0] // parts
    copies = [
        pltpu.make_async_copy(
            hap_hbm.at[pl.ds(k * rows, rows)], hap_ref.at[pl.ds(k * rows, rows)], arrived.at[k]
        )
        for k in range(parts)
    ]
    for copy in copies:
        copy.start()
    out_ref[...] = jnp.zeros_like(out_ref)
    for k, copy in enumerate(copies):
        copy.wait()
        block = hap_ref[k * rows : (k + 1) * rows, :].astype(jnp.float32)
        out_ref[...] += jnp.sum(block, axis=0, keepdims=True)


def load(haplotypes):
    return pl.pallas_call(
        load_kernel,
        in_specs=[pl.BlockSpec(memory_space=pltpu.HBM)],
        out_specs=[pl.BlockSpec(memory_space=pltpu.VMEM)] * 2,
        out_shape=[
            jax.ShapeDtypeStruct(haplotypes.shape, haplotypes.dtype),
            jax.ShapeDtypeStruct((1, haplotypes.shape[1]), jnp.float32),
        ],
        scratch_shapes=[pltpu.SemaphoreType.DMA((4,))],
        compiler_params=pltpu.CompilerParams(vmem_limit_bytes=VMEM_LIMIT),
        name="local_counts",
    )(pltpu.with_memory_space_constraint(haplotypes, pltpu.HBM))


def standardize_part(raw_ref, counts_ref, first, haplo_total):
    frequency, inverse_sd = moments(counts_ref[:, first : first + raw_ref.shape[1]], haplo_total)
    return standardize(raw_ref[...], frequency, inverse_sd)


def own_kernel(
    share, haplo_total, rates, hap_ref, counts_ref,
    std_ref, norm_ref, token_ref, high_ref, send_ref, low_ref, low_send_1, low_send_2,
):
    token_ref[...] = jnp.zeros_like(token_ref)
    std_ref[...] = standardize_part(hap_ref, counts_ref, 0, haplo_total)
    mine = lax.axis_index("samples")
    half = share // 2
    later = std_ref[:, share:]
    send_ref[...] = product(later, std_ref[:, columns(1 - mine, share)]).astype(jnp.bfloat16)
    high_ref[...] = product(later, std_ref[:, columns(mine, share)])
    low = product(std_ref[:, half:share], std_ref[:, :share])
    low_ref[half:, :] = low
    low_send_1[...] = low.astype(jnp.bfloat16)
    low = product(std_ref[:, :half], std_ref[:, :half])
    low_ref[:half, :half] = low
    low_send_2[...] = low.astype(jnp.bfloat16)
    me = lax.axis_index("genome") * lax.axis_size("samples") + mine
    position = (me * share + lax.broadcasted_iota(jnp.int32, (1, share), 1)).astype(jnp.float32) + 1.0
    for k, rate in enumerate(rates):
        norm_ref[k : k + 1, :] = math.expm1(rate) / expm1(position * rate)


def first_kernel(
    share, haplo_total, raw_ref, counts_ref, std_ref, before_ref, token_ref, keep_ref, send_ref
):
    token_ref[...] = before_ref[...]
    later = standardize_part(raw_ref, counts_ref, 0, haplo_total)
    mine = lax.axis_index("samples")
    send_ref[...] = product(later, std_ref[:, columns(1 - mine, share)]).astype(jnp.bfloat16)
    keep_ref[...] = product(later, std_ref[:, columns(mine, share)])


def middle_kernel(
    first, share, haplo_total, raw_ref, counts_ref, std_ref, low_send_1, before_ref,
    token_ref, keep_ref, send_ref, corner_ref, corner_send,
):
    token_ref[...] = before_ref[...]
    later = standardize_part(raw_ref, counts_ref, first, haplo_total)
    keep = product(later, std_ref[:, share:])
    keep_ref[...] = keep
    corner = product(later[:, : share - first], std_ref[:, first:share])
    corner_ref[...] = corner
    corner_send[...] = corner.astype(jnp.bfloat16)
    mine = lax.axis_index("samples")

    @pl.when(mine == 0)
    def _():
        send_ref[...] = keep.astype(jnp.bfloat16)

    @pl.when(mine == 1)
    def _():
        send_ref[...] = low_send_1[...]


def upper_kernel(first, haplo_total, fills, raw_ref, counts_ref, std_ref, before_ref, *refs):
    token_ref, keep_ref, send_ref = refs[len(fills) :]
    token_ref[...] = before_ref[...]
    later = standardize_part(raw_ref, counts_ref, first, haplo_total)
    keep = product(later, std_ref[:, first:])
    keep_ref[...] = keep
    mine = lax.axis_index("samples")

    @pl.when(mine == 0)
    def _():
        send_ref[...] = keep.astype(jnp.bfloat16)

    @pl.when(mine == 1)
    def _():
        for ref, rows, at in zip(refs, *zip(*fills)):
            send_ref[:, at] = ref[rows, :]


def last_kernel(first, haplo_total, raw_ref, counts_ref, std_ref, keep_ref, send_ref):
    later = standardize_part(raw_ref, counts_ref, first, haplo_total)
    keep = product(later, std_ref[:, first:])
    keep_ref[...] = keep
    send_ref[...] = keep.astype(jnp.bfloat16)


def window_sums(total, haplo_total, first_column, first_row, ends):
    correlation = total / haplo_total
    column = first_column + lax.broadcasted_iota(jnp.int32, total.shape, 0)
    row = first_row + lax.broadcasted_iota(jnp.int32, total.shape, 1)
    inside = (column > row) & (column < ends)
    return jnp.sum(jnp.where(inside, correlation * correlation, 0.0), axis=0, keepdims=True)


def local_ends(ends_ref, share):
    start = lax.axis_index("genome") * (lax.axis_size("samples") * share)
    return ends_ref[...] - start


def add_blocks(pieces, refs, share, haplo_total, ends, out_ref):
    mine = lax.axis_index("samples")
    for owner, keep, keep_at, got, got_at, first_column, first_row in pieces:

        def add(keep=keep, keep_at=keep_at, got=got, got_at=got_at, first_column=first_column, first_row=first_row):
            total = refs[keep][keep_at] + refs[got][got_at].astype(jnp.float32)
            start = first_row % share
            inner = slice(start, start + total.shape[1])
            row = mine * share + start
            out_ref[:, inner] += window_sums(total, haplo_total, first_column, row, ends[:, inner])

        if owner is None:
            add()
        else:
            pl.when(mine == owner)(add)


def early_kernel(share, haplo_total, pieces, ends_ref, *refs):
    out_ref = refs[-1]
    out_ref[...] = jnp.zeros_like(out_ref)
    add_blocks(pieces, refs, share, haplo_total, local_ends(ends_ref, share), out_ref)


def rates_of(share, variants):
    return (math.log(0.5) / (4 * share), math.log(0.1) / variants)


def tail_kernel(share, haplo_total, pieces, rates, ends_ref, sums_ref, *refs):
    score_ref, local_ref, last_ref, total_ref = refs[-4:]
    mine = lax.axis_index("samples")
    ends = local_ends(ends_ref, share)
    total_ref[...] = sums_ref[...]
    add_blocks(pieces, refs, share, haplo_total, ends, total_ref)
    row = mine * share + lax.broadcasted_iota(jnp.int32, (1, share), 1)
    counted = jnp.maximum(ends - row - 1, 1).astype(jnp.float32)
    score = total_ref[...] / counted
    score_ref[...] = score
    blocks = share // LANES
    stacked = jnp.concatenate(
        [score[:, b * LANES : (b + 1) * LANES] for b in range(blocks)]
        + ([jnp.zeros(((-blocks) % 8, LANES), jnp.float32)] if blocks % 8 else []),
        axis=0,
    )
    source = lax.broadcasted_iota(jnp.int32, (LANES, LANES), 0)
    target = lax.broadcasted_iota(jnp.int32, (LANES, LANES), 1)
    lag = (target - source).astype(jnp.float32)
    lane = lax.broadcasted_iota(jnp.int32, (1, LANES), 1).astype(jnp.float32)
    lasts = []
    for k, rate in enumerate(rates):
        weight = jnp.where(lag >= 0.0, jnp.exp(jnp.maximum(lag, 0.0) * rate), 0.0)
        to_end = jnp.exp((LANES - 1.0 - source.astype(jnp.float32)) * rate)
        inner, ending = (
            lax.dot_general(
                stacked,
                w,
                (((1,), (0,)), ((), ())),
                precision=lax.Precision.HIGHEST,
                preferred_element_type=jnp.float32,
            )
            for w in (weight, to_end)
        )
        fall = jnp.exp((lane + 1.0) * rate)
        block_fall = math.exp(LANES * rate)
        carry = jnp.zeros((1, LANES), jnp.float32)
        for b in range(blocks):
            local_ref[k : k + 1, b * LANES : (b + 1) * LANES] = inner[b : b + 1, :] + carry * fall
            carry = ending[b : b + 1, :] + carry * block_fall
        lasts.append(carry)
    tile_lane = lax.broadcasted_iota(jnp.int32, last_ref.shape, 1)
    last_ref[...] = jnp.where(tile_lane == 0, lasts[0], jnp.where(tile_lane == 1, lasts[1], 0.0))


def finish_kernel(rates, local_ref, table_ref, norm_ref, profile_ref):
    share = local_ref.shape[1]
    peers = table_ref.shape[0]
    me = lax.axis_index("genome") * lax.axis_size("samples") + lax.axis_index("samples")
    peer = lax.broadcasted_iota(jnp.int32, (peers, LANES), 0)
    gap = ((me - 1 - peer) * share).astype(jnp.float32)
    step = lax.broadcasted_iota(jnp.int32, (1, share), 1).astype(jnp.float32)
    for k, rate in enumerate(rates):
        weight = jnp.where(peer < me, jnp.exp(jnp.maximum(gap, 0.0) * rate), 0.0)
        incoming = jnp.sum(weight * table_ref[...], axis=0, keepdims=True)[:, k : k + 1]
        smoothed = local_ref[k : k + 1, :] + incoming * jnp.exp((step + 1.0) * rate)
        profile_ref[k : k + 1, :] = smoothed * norm_ref[k : k + 1, :]


def per_device(haplotypes, window_ends):
    samples = lax.axis_size("samples")
    genome = lax.axis_size("genome")
    depth, width = haplotypes.shape
    share = width // samples
    haplo_total = float(depth * samples)
    rates = rates_of(share, width * genome)
    back = [(i + 1, i) for i in range(genome - 1)]
    ends = window_ends[None]
    f32, bf16 = jnp.float32, jnp.bfloat16
    unit = width // 8
    firsts = [unit * sum(EIGHTHS[:c]) for c in range(len(EIGHTHS))]
    sizes = [unit * e for e in EIGHTHS]

    def shifted(array, c):
        return lax.ppermute(array[:, firsts[c] : firsts[c] + sizes[c]], "genome", back)

    raws = [shifted(haplotypes, 0)]
    haplotypes, counts = load(haplotypes)
    raws += [shifted(haplotypes, c) for c in range(1, len(EIGHTHS))]
    if samples == 2:
        counts = counts + lax.ppermute(counts, "samples", [(0, 1), (1, 0)])
    else:
        counts = lax.psum(counts, "samples")
    next_counts = lax.ppermute(counts, "genome", back)

    def swap(send):
        return lax.ppermute(send, "samples", [(0, 1), (1, 0)])

    tails, tail_pieces = [], []
    token_type = ((8, LANES), f32)
    if samples == 2:
        half, u, whole = share // 2, unit, slice(None)
        standard, norm, token, high, send, low, low_send_1, low_send_2 = call(
            functools.partial(own_kernel, share, haplo_total, rates),
            [((depth, width), bf16), ((2, share), f32), token_type]
            + [((share, share), f32), ((share, share), bf16), ((share, share), f32)]
            + [((half, share), bf16), ((half, half), bf16)],
            haplotypes,
            counts,
        )
        got_0 = swap(send)
        token, keep_1, send = call(
            functools.partial(first_kernel, share, haplo_total),
            [token_type, ((3 * u, share), f32), ((3 * u, share), bf16)],
            raws[0],
            next_counts,
            standard,
            token,
        )
        got_1 = swap(send)
        token, keep_2, send, corner, corner_send = call(
            functools.partial(middle_kernel, firsts[1], share, haplo_total),
            [token_type, ((2 * u, share), f32), ((2 * u, share), bf16), ((u, u), f32), ((u, u), bf16)],
            raws[1],
            next_counts,
            standard,
            low_send_1,
            token,
        )
        got_2 = swap(send)
        first_unit, second_unit = slice(0, u), slice(u, None)
        lower, upper = slice(0, half), slice(half, None)
        tails = [low, corner]
        for c, fills, extra in (
            (2, [(first_unit, lower), (whole, upper)], [low_send_2, corner_send]),
            (3, [(second_unit, lower)], [low_send_2]),
        ):
            shape = (u, width - firsts[c])
            token, keep, send = call(
                functools.partial(upper_kernel, firsts[c], haplo_total, fills),
                [token_type, (shape, f32), (shape, bf16)],
                raws[c],
                next_counts,
                standard,
                token,
                *extra,
            )
            tails += [keep, swap(send)]
        pieces = [
            (None, 0, (whole, whole), 1, (whole, whole), share, 0),
            (None, 2, (whole, whole), 3, (whole, whole), width, 0),
            (0, 4, (slice(half, None), whole), 6, (whole, whole), half, 0),
            (1, 5, (whole, whole), 6, (whole, whole), width + firsts[1], share),
        ]
        (sums,) = call(
            functools.partial(early_kernel, share, haplo_total, pieces),
            [((1, share), f32)],
            ends,
            high,
            got_0,
            keep_1,
            got_1,
            low,
            keep_2,
            got_2,
        )
        keep, send = call(
            functools.partial(last_kernel, firsts[4], haplo_total),
            [((u, u), f32), ((u, u), bf16)],
            raws[4],
            next_counts,
            standard,
        )
        tails += [keep, swap(send)]
        tail_pieces = [
            (0, 0, (first_unit, lower), 3, (whole, lower), 0, 0),
            (0, 0, (slice(u, half), lower), 5, (whole, lower), u, 0),
            (0, 1, (whole, whole), 3, (whole, upper), width + firsts[1], firsts[1]),
        ] + [
            (1, 2 * c - 2, (whole, whole), 2 * c - 1, (whole, whole), width + firsts[c], firsts[c])
            for c in (2, 3, 4)
        ]
    else:
        frequency, inverse_sd = moments(counts, haplo_total)
        standard = standardize(haplotypes, frequency, inverse_sd)
        frequency, inverse_sd = moments(next_counts, haplo_total)
        later = standardize(jnp.concatenate(raws, axis=1), frequency, inverse_sd)
        total = lax.psum_scatter(
            product(jnp.concatenate([standard, later], axis=1), standard),
            "samples",
            scatter_dimension=1,
            tiled=True,
        )
        me = lax.axis_index("genome") * samples + lax.axis_index("samples")
        position = (me * share + jnp.arange(share, dtype=jnp.int32)).astype(f32) + 1.0
        log_rates = jnp.array(rates, f32)[:, None]
        norm = jnp.expm1(log_rates) / jnp.expm1(position[None] * log_rates)
        sums = window_sums(
            total,
            haplo_total,
            0,
            lax.axis_index("samples") * share,
            ends - lax.axis_index("genome") * width,
        )

    score, local, last, _ = call(
        functools.partial(tail_kernel, share, haplo_total, tail_pieces, rates),
        [((1, share), f32), ((2, share), f32), ((genome * samples, LANES), f32), ((1, share), f32)],
        ends,
        sums,
        *tails,
    )
    table = lax.all_to_all(last[:, None], ("genome", "samples"), 0, 0, tiled=True)[:, 0]
    (profile,) = call(
        functools.partial(finish_kernel, rates), [((2, share), f32)], local, table, norm
    )
    return score[0], profile


def solution(mesh):
    return jax.shard_map(
        per_device,
        mesh=mesh,
        in_specs=(P("samples", "genome"), P(("genome", "samples"))),
        out_specs=(P(("genome", "samples")), P(None, ("genome", "samples"))),
        check_vma=False,
    )
```

```python
import functools
import math

import jax
import jax.numpy as jnp
from jax import lax
from jax.experimental import pallas as pl
from jax.experimental.pallas import tpu as pltpu
from jax.sharding import PartitionSpec as P


LANES = 128
EIGHTHS = (3, 2, 1, 1, 1)
VMEM_LIMIT = 20 * 2**20
variance_floor = 0.01


def standardize(alleles, frequency, inverse_sd):
    return ((alleles.astype(jnp.float32) - frequency) * inverse_sd).astype(jnp.bfloat16)


def product(left, right):
    return lax.dot_general(
        left, right, (((0,), (0,)), ((), ())), preferred_element_type=jnp.float32
    )


def moments(counts, haplo_total):
    frequency = counts / haplo_total
    return frequency, lax.rsqrt(jnp.maximum(frequency * (1.0 - frequency), variance_floor))


def call(kernel, shapes, *arrays):
    return pl.pallas_call(
        kernel,
        in_specs=[pl.BlockSpec(memory_space=pltpu.VMEM)] * len(arrays),
        out_specs=[pl.BlockSpec(memory_space=pltpu.VMEM)] * len(shapes),
        out_shape=[jax.ShapeDtypeStruct(s, t) for s, t in shapes],
        compiler_params=pltpu.CompilerParams(vmem_limit_bytes=VMEM_LIMIT),
    )(*arrays)


def columns(index, width):
    return pl.ds(pl.multiple_of(index * width, LANES), width)


def expm1(x):
    series = jnp.ones_like(x)
    for n in range(9, 1, -1):
        series = 1.0 + series * (x * (1.0 / n))
    return jnp.where(x > -0.35, x * series, jnp.exp(x) - 1.0)


def load_kernel(hap_hbm, hap_ref, out_ref, arrived):
    parts = arrived.shape[0]
    rows = hap_ref.shape[0] // parts
    copies = [
        pltpu.make_async_copy(
            hap_hbm.at[pl.ds(k * rows, rows)], hap_ref.at[pl.ds(k * rows, rows)], arrived.at[k]
        )
        for k in range(parts)
    ]
    for copy in copies:
        copy.start()
    out_ref[...] = jnp.zeros_like(out_ref)
    for k, copy in enumerate(copies):
        copy.wait()
        block = hap_ref[k * rows : (k + 1) * rows, :].astype(jnp.float32)
        out_ref[...] += jnp.sum(block, axis=0, keepdims=True)


def load(haplotypes):
    return pl.pallas_call(
        load_kernel,
        in_specs=[pl.BlockSpec(memory_space=pltpu.HBM)],
        out_specs=[pl.BlockSpec(memory_space=pltpu.VMEM)] * 2,
        out_shape=[
            jax.ShapeDtypeStruct(haplotypes.shape, haplotypes.dtype),
            jax.ShapeDtypeStruct((1, haplotypes.shape[1]), jnp.float32),
        ],
        scratch_shapes=[pltpu.SemaphoreType.DMA((4,))],
        compiler_params=pltpu.CompilerParams(vmem_limit_bytes=VMEM_LIMIT),
        name="local_counts",
    )(pltpu.with_memory_space_constraint(haplotypes, pltpu.HBM))


def standardize_part(raw_ref, counts_ref, first, haplo_total):
    frequency, inverse_sd = moments(counts_ref[:, first : first + raw_ref.shape[1]], haplo_total)
    return standardize(raw_ref[...], frequency, inverse_sd)


def own_kernel(
    share, haplo_total, rates, hap_ref, counts_ref,
    std_ref, norm_ref, decay_ref, peer_ref, token_ref,
    high_ref, send_ref, low_ref, low_send_1, low_send_2,
):
    token_ref[...] = jnp.zeros_like(token_ref)
    std_ref[...] = standardize_part(hap_ref, counts_ref, 0, haplo_total)
    mine = lax.axis_index("samples")
    half = share // 2
    later = std_ref[:, share:]
    send_ref[...] = product(later, std_ref[:, columns(1 - mine, share)]).astype(jnp.bfloat16)
    high_ref[...] = product(later, std_ref[:, columns(mine, share)])
    low = product(std_ref[:, half:share], std_ref[:, :share])
    low_ref[half:, :] = low
    low_send_1[...] = low.astype(jnp.bfloat16)
    low = product(std_ref[:, :half], std_ref[:, :half])
    low_ref[:half, :half] = low
    low_send_2[...] = low.astype(jnp.bfloat16)
    me = lax.axis_index("genome") * lax.axis_size("samples") + mine
    step = lax.broadcasted_iota(jnp.int32, (1, share), 1)
    position = (me * share + step).astype(jnp.float32) + 1.0
    source = lax.broadcasted_iota(jnp.int32, (LANES, LANES), 0)
    target = lax.broadcasted_iota(jnp.int32, (LANES, LANES), 1)
    lag = (target - source).astype(jnp.float32)
    to_end = (LANES - 1 - source).astype(jnp.float32)
    peer = lax.broadcasted_iota(jnp.int32, peer_ref.shape, 0)
    peer_lane = lax.broadcasted_iota(jnp.int32, peer_ref.shape, 1)
    gap = jnp.maximum((me - 1 - peer) * share, 0).astype(jnp.float32)
    peer_weight = jnp.zeros(peer_ref.shape, jnp.float32)
    for k, rate in enumerate(rates):
        norm = math.expm1(rate) / expm1(position * rate)
        norm_ref[k : k + 1, :] = norm
        norm_ref[2 + k : 3 + k, :] = norm * jnp.exp((step.astype(jnp.float32) + 1.0) * rate)
        at = 2 * k * LANES
        decay_ref[:, at : at + LANES] = jnp.where(
            lag >= 0.0, jnp.exp(jnp.maximum(lag, 0.0) * rate), 0.0
        )
        decay_ref[:, at + LANES : at + 2 * LANES] = jnp.exp(to_end * rate)
        used = (peer < me) & (peer_lane == k)
        peer_weight = peer_weight + jnp.where(used, jnp.exp(gap * rate), 0.0)
    peer_ref[...] = peer_weight


def first_kernel(
    share, haplo_total, raw_ref, counts_ref, std_ref, before_ref, token_ref, keep_ref, send_ref
):
    token_ref[...] = before_ref[...]
    later = standardize_part(raw_ref, counts_ref, 0, haplo_total)
    mine = lax.axis_index("samples")
    send_ref[...] = product(later, std_ref[:, columns(1 - mine, share)]).astype(jnp.bfloat16)
    keep_ref[...] = product(later, std_ref[:, columns(mine, share)])


def middle_kernel(
    first, share, haplo_total, raw_ref, counts_ref, std_ref, low_send_1, before_ref,
    token_ref, keep_ref, send_ref, corner_ref, corner_send,
):
    token_ref[...] = before_ref[...]
    later = standardize_part(raw_ref, counts_ref, first, haplo_total)
    keep = product(later, std_ref[:, share:])
    keep_ref[...] = keep
    corner = product(later[:, : share - first], std_ref[:, first:share])
    corner_ref[...] = corner
    corner_send[...] = corner.astype(jnp.bfloat16)
    mine = lax.axis_index("samples")

    @pl.when(mine == 0)
    def _():
        send_ref[...] = keep.astype(jnp.bfloat16)

    @pl.when(mine == 1)
    def _():
        send_ref[...] = low_send_1[...]


def upper_kernel(first, haplo_total, fills, raw_ref, counts_ref, std_ref, before_ref, *refs):
    token_ref, keep_ref, send_ref = refs[len(fills) :]
    token_ref[...] = before_ref[...]
    later = standardize_part(raw_ref, counts_ref, first, haplo_total)
    keep = product(later, std_ref[:, first:])
    keep_ref[...] = keep
    mine = lax.axis_index("samples")

    @pl.when(mine == 0)
    def _():
        send_ref[...] = keep.astype(jnp.bfloat16)

    @pl.when(mine == 1)
    def _():
        for ref, rows, at in zip(refs, *zip(*fills)):
            send_ref[:, at] = ref[rows, :]


def last_kernel(first, haplo_total, raw_ref, counts_ref, std_ref, keep_ref, send_ref):
    later = standardize_part(raw_ref, counts_ref, first, haplo_total)
    keep = product(later, std_ref[:, first:])
    keep_ref[...] = keep
    send_ref[...] = keep.astype(jnp.bfloat16)


def window_sums(total, haplo_total, first_column, first_row, ends):
    correlation = total / haplo_total
    column = first_column + lax.broadcasted_iota(jnp.int32, total.shape, 0)
    row = first_row + lax.broadcasted_iota(jnp.int32, total.shape, 1)
    inside = (column > row) & (column < ends)
    return jnp.sum(jnp.where(inside, correlation * correlation, 0.0), axis=0, keepdims=True)


def local_ends(ends_ref, share):
    start = lax.axis_index("genome") * (lax.axis_size("samples") * share)
    return ends_ref[...] - start


def add_blocks(pieces, refs, share, haplo_total, ends, out_ref):
    mine = lax.axis_index("samples")
    for owner, keep, keep_at, got, got_at, first_column, first_row in pieces:

        def add(keep=keep, keep_at=keep_at, got=got, got_at=got_at, first_column=first_column, first_row=first_row):
            total = refs[keep][keep_at] + refs[got][got_at].astype(jnp.float32)
            start = first_row % share
            inner = slice(start, start + total.shape[1])
            row = mine * share + start
            out_ref[:, inner] += window_sums(total, haplo_total, first_column, row, ends[:, inner])

        if owner is None:
            add()
        else:
            pl.when(mine == owner)(add)


def early_kernel(share, haplo_total, pieces, ends_ref, *refs):
    out_ref = refs[-1]
    out_ref[...] = jnp.zeros_like(out_ref)
    add_blocks(pieces, refs, share, haplo_total, local_ends(ends_ref, share), out_ref)


def rates_of(share, variants):
    return (math.log(0.5) / (4 * share), math.log(0.1) / variants)


def tail_kernel(share, haplo_total, pieces, rates, ends_ref, sums_ref, decay_ref, *refs):
    score_ref, local_ref, last_ref, total_ref = refs[-4:]
    mine = lax.axis_index("samples")
    ends = local_ends(ends_ref, share)
    total_ref[...] = sums_ref[...]
    add_blocks(pieces, refs, share, haplo_total, ends, total_ref)
    row = mine * share + lax.broadcasted_iota(jnp.int32, (1, share), 1)
    counted = jnp.maximum(ends - row - 1, 1).astype(jnp.float32)
    score = total_ref[...] / counted
    score_ref[...] = score
    blocks = share // LANES
    stacked = jnp.concatenate(
        [score[:, b * LANES : (b + 1) * LANES] for b in range(blocks)]
        + ([jnp.zeros(((-blocks) % 8, LANES), jnp.float32)] if blocks % 8 else []),
        axis=0,
    )
    lane = lax.broadcasted_iota(jnp.int32, (1, LANES), 1).astype(jnp.float32)
    within = lax.dot_general(
        stacked,
        decay_ref[...],
        (((1,), (0,)), ((), ())),
        precision=lax.Precision.HIGHEST,
        preferred_element_type=jnp.float32,
    )
    lasts = []
    for k, rate in enumerate(rates):
        at = 2 * k * LANES
        inner, ending = within[:, at : at + LANES], within[:, at + LANES : at + 2 * LANES]
        fall = jnp.exp((lane + 1.0) * rate)
        block_fall = math.exp(LANES * rate)
        carry = jnp.zeros((1, LANES), jnp.float32)
        for b in range(blocks):
            local_ref[k : k + 1, b * LANES : (b + 1) * LANES] = inner[b : b + 1, :] + carry * fall
            carry = ending[b : b + 1, :] + carry * block_fall
        lasts.append(carry)
    tile_lane = lax.broadcasted_iota(jnp.int32, last_ref.shape, 1)
    last_ref[...] = jnp.where(tile_lane == 0, lasts[0], jnp.where(tile_lane == 1, lasts[1], 0.0))


def finish_kernel(local_ref, table_ref, norm_ref, peer_ref, profile_ref):
    incoming = jnp.sum(peer_ref[...] * table_ref[...], axis=0, keepdims=True)
    for k in range(2):
        profile_ref[k : k + 1, :] = (
            local_ref[k : k + 1, :] * norm_ref[k : k + 1, :]
            + incoming[:, k : k + 1] * norm_ref[2 + k : 3 + k, :]
        )


def peer_constants(rates, share, peers, me):
    f32 = jnp.float32
    log_rates = jnp.array(rates, f32)[:, None]
    step = jnp.arange(share, dtype=jnp.int32)
    position = (me * share + step).astype(f32)[None] + 1.0
    norm = jnp.expm1(log_rates) / jnp.expm1(position * log_rates)
    fall = jnp.exp((step.astype(f32)[None] + 1.0) * log_rates)
    lane = jnp.arange(LANES, dtype=f32)
    lag = lane[None] - lane[:, None]
    decays = []
    for rate in rates:
        decays.append(jnp.where(lag >= 0.0, jnp.exp(jnp.maximum(lag, 0.0) * rate), 0.0))
        decays.append(jnp.broadcast_to(jnp.exp((LANES - 1.0 - lane[:, None]) * rate), lag.shape))
    peer = jnp.arange(peers, dtype=jnp.int32)
    gap = jnp.maximum((me - 1 - peer) * share, 0).astype(f32)
    weight = jnp.where(peer[None] < me, jnp.exp(gap[None] * log_rates), 0.0).T
    weight = jnp.pad(weight, ((0, 0), (0, LANES - len(rates))))
    return jnp.concatenate([norm, norm * fall]), jnp.concatenate(decays, axis=1), weight


def per_device(haplotypes, window_ends):
    samples = lax.axis_size("samples")
    genome = lax.axis_size("genome")
    depth, width = haplotypes.shape
    share = width // samples
    haplo_total = float(depth * samples)
    rates = rates_of(share, width * genome)
    back = [(i + 1, i) for i in range(genome - 1)]
    ends = window_ends[None]
    f32, bf16 = jnp.float32, jnp.bfloat16
    unit = width // 8
    firsts = [unit * sum(EIGHTHS[:c]) for c in range(len(EIGHTHS))]
    sizes = [unit * e for e in EIGHTHS]

    def shifted(array, c):
        return lax.ppermute(array[:, firsts[c] : firsts[c] + sizes[c]], "genome", back)

    raws = [shifted(haplotypes, 0)]
    haplotypes, counts = load(haplotypes)
    raws += [shifted(haplotypes, c) for c in range(1, len(EIGHTHS))]
    if samples == 2:
        counts = counts + lax.ppermute(counts, "samples", [(0, 1), (1, 0)])
    else:
        counts = lax.psum(counts, "samples")
    next_counts = lax.ppermute(counts, "genome", back)

    def swap(send):
        return lax.ppermute(send, "samples", [(0, 1), (1, 0)])

    tails, tail_pieces = [], []
    token_type = ((8, LANES), f32)
    if samples == 2:
        half, u, whole = share // 2, unit, slice(None)
        standard, norm, decay, peer, token, high, send, low, low_send_1, low_send_2 = call(
            functools.partial(own_kernel, share, haplo_total, rates),
            [((depth, width), bf16), ((4, share), f32), ((LANES, 4 * LANES), f32)]
            + [((genome * samples, LANES), f32), token_type]
            + [((share, share), f32), ((share, share), bf16), ((share, share), f32)]
            + [((half, share), bf16), ((half, half), bf16)],
            haplotypes,
            counts,
        )
        got_0 = swap(send)
        token, keep_1, send = call(
            functools.partial(first_kernel, share, haplo_total),
            [token_type, ((3 * u, share), f32), ((3 * u, share), bf16)],
            raws[0],
            next_counts,
            standard,
            token,
        )
        got_1 = swap(send)
        token, keep_2, send, corner, corner_send = call(
            functools.partial(middle_kernel, firsts[1], share, haplo_total),
            [token_type, ((2 * u, share), f32), ((2 * u, share), bf16), ((u, u), f32), ((u, u), bf16)],
            raws[1],
            next_counts,
            standard,
            low_send_1,
            token,
        )
        got_2 = swap(send)
        first_unit, second_unit = slice(0, u), slice(u, None)
        lower, upper = slice(0, half), slice(half, None)
        tails = [low, corner]
        for c, fills, extra in (
            (2, [(first_unit, lower), (whole, upper)], [low_send_2, corner_send]),
            (3, [(second_unit, lower)], [low_send_2]),
        ):
            shape = (u, width - firsts[c])
            token, keep, send = call(
                functools.partial(upper_kernel, firsts[c], haplo_total, fills),
                [token_type, (shape, f32), (shape, bf16)],
                raws[c],
                next_counts,
                standard,
                token,
                *extra,
            )
            tails += [keep, swap(send)]
        pieces = [
            (None, 0, (whole, whole), 1, (whole, whole), share, 0),
            (None, 2, (whole, whole), 3, (whole, whole), width, 0),
            (0, 4, (slice(half, None), whole), 6, (whole, whole), half, 0),
            (1, 5, (whole, whole), 6, (whole, whole), width + firsts[1], share),
        ]
        (sums,) = call(
            functools.partial(early_kernel, share, haplo_total, pieces),
            [((1, share), f32)],
            ends,
            high,
            got_0,
            keep_1,
            got_1,
            low,
            keep_2,
            got_2,
        )
        keep, send = call(
            functools.partial(last_kernel, firsts[4], haplo_total),
            [((u, u), f32), ((u, u), bf16)],
            raws[4],
            next_counts,
            standard,
        )
        tails += [keep, swap(send)]
        tail_pieces = [
            (0, 0, (first_unit, lower), 3, (whole, lower), 0, 0),
            (0, 0, (slice(u, half), lower), 5, (whole, lower), u, 0),
            (0, 1, (whole, whole), 3, (whole, upper), width + firsts[1], firsts[1]),
        ] + [
            (1, 2 * c - 2, (whole, whole), 2 * c - 1, (whole, whole), width + firsts[c], firsts[c])
            for c in (2, 3, 4)
        ]
    else:
        frequency, inverse_sd = moments(counts, haplo_total)
        standard = standardize(haplotypes, frequency, inverse_sd)
        frequency, inverse_sd = moments(next_counts, haplo_total)
        later = standardize(jnp.concatenate(raws, axis=1), frequency, inverse_sd)
        total = lax.psum_scatter(
            product(jnp.concatenate([standard, later], axis=1), standard),
            "samples",
            scatter_dimension=1,
            tiled=True,
        )
        me = lax.axis_index("genome") * samples + lax.axis_index("samples")
        norm, decay, peer = peer_constants(rates, share, genome * samples, me)
        sums = window_sums(
            total,
            haplo_total,
            0,
            lax.axis_index("samples") * share,
            ends - lax.axis_index("genome") * width,
        )

    score, local, last, _ = call(
        functools.partial(tail_kernel, share, haplo_total, tail_pieces, rates),
        [((1, share), f32), ((2, share), f32), ((genome * samples, LANES), f32), ((1, share), f32)],
        ends,
        sums,
        decay,
        *tails,
    )
    table = lax.all_to_all(last[:, None], ("genome", "samples"), 0, 0, tiled=True)[:, 0]
    (profile,) = call(finish_kernel, [((2, share), f32)], local, table, norm, peer)
    return score[0], profile


def solution(mesh):
    return jax.shard_map(
        per_device,
        mesh=mesh,
        in_specs=(P("samples", "genome"), P(("genome", "samples"))),
        out_specs=(P(("genome", "samples")), P(None, ("genome", "samples"))),
        check_vma=False,
    )
```

```python
import functools
import math

import jax
import jax.numpy as jnp
from jax import lax
from jax.experimental import pallas as pl
from jax.experimental.pallas import tpu as pltpu
from jax.sharding import PartitionSpec as P


LANES = 128
EIGHTHS = (3, 2, 1, 1, 1)
VMEM_LIMIT = 20 * 2**20
variance_floor = 0.01


def standardize(alleles, frequency, inverse_sd):
    return ((alleles.astype(jnp.float32) - frequency) * inverse_sd).astype(jnp.bfloat16)


def product(left, right):
    return lax.dot_general(
        left, right, (((0,), (0,)), ((), ())), preferred_element_type=jnp.float32
    )


def moments(counts, haplo_total):
    frequency = counts / haplo_total
    return frequency, lax.rsqrt(jnp.maximum(frequency * (1.0 - frequency), variance_floor))


def call(kernel, shapes, *arrays):
    return pl.pallas_call(
        kernel,
        in_specs=[pl.BlockSpec(memory_space=pltpu.VMEM)] * len(arrays),
        out_specs=[pl.BlockSpec(memory_space=pltpu.VMEM)] * len(shapes),
        out_shape=[jax.ShapeDtypeStruct(s, t) for s, t in shapes],
        compiler_params=pltpu.CompilerParams(vmem_limit_bytes=VMEM_LIMIT),
    )(*arrays)


def columns(index, width):
    return pl.ds(pl.multiple_of(index * width, LANES), width)


def expm1(x):
    series = jnp.ones_like(x)
    for n in range(9, 1, -1):
        series = 1.0 + series * (x * (1.0 / n))
    return jnp.where(x > -0.35, x * series, jnp.exp(x) - 1.0)


def load_kernel(hap_hbm, hap_ref, out_ref, arrived):
    parts = arrived.shape[0]
    rows = hap_ref.shape[0] // parts
    copies = [
        pltpu.make_async_copy(
            hap_hbm.at[pl.ds(k * rows, rows)], hap_ref.at[pl.ds(k * rows, rows)], arrived.at[k]
        )
        for k in range(parts)
    ]
    for copy in copies:
        copy.start()
    out_ref[...] = jnp.zeros_like(out_ref)
    for k, copy in enumerate(copies):
        copy.wait()
        block = hap_ref[k * rows : (k + 1) * rows, :].astype(jnp.float32)
        out_ref[...] += jnp.sum(block, axis=0, keepdims=True)


def cut_kernel(first, hap_hbm, out_ref, arrived):
    parts = arrived.shape[0]
    rows, size = out_ref.shape[0] // parts, out_ref.shape[1]
    copies = [
        pltpu.make_async_copy(
            hap_hbm.at[pl.ds(k * rows, rows), pl.ds(first, size)],
            out_ref.at[pl.ds(k * rows, rows)],
            arrived.at[k],
        )
        for k in range(parts)
    ]
    for copy in copies:
        copy.start()
    for copy in copies:
        copy.wait()


def cut(haplotypes, first, size):
    return pl.pallas_call(
        functools.partial(cut_kernel, first),
        in_specs=[pl.BlockSpec(memory_space=pltpu.HBM)],
        out_specs=pl.BlockSpec(memory_space=pltpu.VMEM),
        out_shape=jax.ShapeDtypeStruct((haplotypes.shape[0], size), haplotypes.dtype),
        scratch_shapes=[pltpu.SemaphoreType.DMA((4,))],
        compiler_params=pltpu.CompilerParams(vmem_limit_bytes=VMEM_LIMIT),
        name="cut",
    )(pltpu.with_memory_space_constraint(haplotypes, pltpu.HBM))


def load(haplotypes):
    return pl.pallas_call(
        load_kernel,
        in_specs=[pl.BlockSpec(memory_space=pltpu.HBM)],
        out_specs=[pl.BlockSpec(memory_space=pltpu.VMEM)] * 2,
        out_shape=[
            jax.ShapeDtypeStruct(haplotypes.shape, haplotypes.dtype),
            jax.ShapeDtypeStruct((1, haplotypes.shape[1]), jnp.float32),
        ],
        scratch_shapes=[pltpu.SemaphoreType.DMA((4,))],
        compiler_params=pltpu.CompilerParams(vmem_limit_bytes=VMEM_LIMIT),
        name="local_counts",
    )(pltpu.with_memory_space_constraint(haplotypes, pltpu.HBM))


def standardize_part(raw_ref, counts_ref, first, haplo_total):
    frequency, inverse_sd = moments(counts_ref[:, first : first + raw_ref.shape[1]], haplo_total)
    return standardize(raw_ref[...], frequency, inverse_sd)


def own_kernel(
    share, haplo_total, rates, hap_ref, counts_ref,
    std_ref, norm_ref, decay_ref, peer_ref, token_ref,
    high_ref, send_ref, low_ref, low_send_1, low_send_2,
):
    token_ref[...] = jnp.zeros_like(token_ref)
    std_ref[...] = standardize_part(hap_ref, counts_ref, 0, haplo_total)
    mine = lax.axis_index("samples")
    half = share // 2
    later = std_ref[:, share:]
    send_ref[...] = product(later, std_ref[:, columns(1 - mine, share)]).astype(jnp.bfloat16)
    high_ref[...] = product(later, std_ref[:, columns(mine, share)])
    low = product(std_ref[:, half:share], std_ref[:, :share])
    low_ref[half:, :] = low
    low_send_1[...] = low.astype(jnp.bfloat16)
    low = product(std_ref[:, :half], std_ref[:, :half])
    low_ref[:half, :half] = low
    low_send_2[...] = low.astype(jnp.bfloat16)
    me = lax.axis_index("genome") * lax.axis_size("samples") + mine
    step = lax.broadcasted_iota(jnp.int32, (1, share), 1)
    position = (me * share + step).astype(jnp.float32) + 1.0
    source = lax.broadcasted_iota(jnp.int32, (LANES, LANES), 0)
    target = lax.broadcasted_iota(jnp.int32, (LANES, LANES), 1)
    lag = (target - source).astype(jnp.float32)
    to_end = (LANES - 1 - source).astype(jnp.float32)
    peer = lax.broadcasted_iota(jnp.int32, peer_ref.shape, 0)
    peer_lane = lax.broadcasted_iota(jnp.int32, peer_ref.shape, 1)
    gap = jnp.maximum((me - 1 - peer) * share, 0).astype(jnp.float32)
    peer_weight = jnp.zeros(peer_ref.shape, jnp.float32)
    for k, rate in enumerate(rates):
        norm = math.expm1(rate) / expm1(position * rate)
        norm_ref[k : k + 1, :] = norm
        norm_ref[2 + k : 3 + k, :] = norm * jnp.exp((step.astype(jnp.float32) + 1.0) * rate)
        at = 2 * k * LANES
        decay_ref[:, at : at + LANES] = jnp.where(
            lag >= 0.0, jnp.exp(jnp.maximum(lag, 0.0) * rate), 0.0
        )
        decay_ref[:, at + LANES : at + 2 * LANES] = jnp.exp(to_end * rate)
        used = (peer < me) & (peer_lane == k)
        peer_weight = peer_weight + jnp.where(used, jnp.exp(gap * rate), 0.0)
    peer_ref[...] = peer_weight


def first_kernel(
    share, haplo_total, raw_ref, counts_ref, std_ref, before_ref, token_ref, keep_ref, send_ref
):
    token_ref[...] = before_ref[...]
    later = standardize_part(raw_ref, counts_ref, 0, haplo_total)
    mine = lax.axis_index("samples")
    send_ref[...] = product(later, std_ref[:, columns(1 - mine, share)]).astype(jnp.bfloat16)
    keep_ref[...] = product(later, std_ref[:, columns(mine, share)])


def middle_kernel(
    first, share, haplo_total, raw_ref, counts_ref, std_ref, low_send_1, before_ref,
    token_ref, keep_ref, send_ref, corner_ref, corner_send,
):
    token_ref[...] = before_ref[...]
    later = standardize_part(raw_ref, counts_ref, first, haplo_total)
    keep = product(later, std_ref[:, share:])
    keep_ref[...] = keep
    corner = product(later[:, : share - first], std_ref[:, first:share])
    corner_ref[...] = corner
    corner_send[...] = corner.astype(jnp.bfloat16)
    mine = lax.axis_index("samples")

    @pl.when(mine == 0)
    def _():
        send_ref[...] = keep.astype(jnp.bfloat16)

    @pl.when(mine == 1)
    def _():
        send_ref[...] = low_send_1[...]


def upper_kernel(first, haplo_total, fills, raw_ref, counts_ref, std_ref, before_ref, *refs):
    token_ref, keep_ref, send_ref = refs[len(fills) :]
    token_ref[...] = before_ref[...]
    later = standardize_part(raw_ref, counts_ref, first, haplo_total)
    keep = product(later, std_ref[:, first:])
    keep_ref[...] = keep
    mine = lax.axis_index("samples")

    @pl.when(mine == 0)
    def _():
        send_ref[...] = keep.astype(jnp.bfloat16)

    @pl.when(mine == 1)
    def _():
        for ref, rows, at in zip(refs, *zip(*fills)):
            send_ref[:, at] = ref[rows, :]


def last_kernel(first, haplo_total, raw_ref, counts_ref, std_ref, keep_ref, send_ref):
    later = standardize_part(raw_ref, counts_ref, first, haplo_total)
    keep = product(later, std_ref[:, first:])
    keep_ref[...] = keep
    send_ref[...] = keep.astype(jnp.bfloat16)


def window_sums(total, haplo_total, first_column, first_row, ends):
    correlation = total / haplo_total
    column = first_column + lax.broadcasted_iota(jnp.int32, total.shape, 0)
    row = first_row + lax.broadcasted_iota(jnp.int32, total.shape, 1)
    inside = (column > row) & (column < ends)
    return jnp.sum(jnp.where(inside, correlation * correlation, 0.0), axis=0, keepdims=True)


def local_ends(ends_ref, share):
    start = lax.axis_index("genome") * (lax.axis_size("samples") * share)
    return ends_ref[...] - start


def add_blocks(pieces, refs, share, haplo_total, ends, out_ref):
    mine = lax.axis_index("samples")
    for owner, keep, keep_at, got, got_at, first_column, first_row in pieces:

        def add(keep=keep, keep_at=keep_at, got=got, got_at=got_at, first_column=first_column, first_row=first_row):
            total = refs[keep][keep_at] + refs[got][got_at].astype(jnp.float32)
            start = first_row % share
            inner = slice(start, start + total.shape[1])
            row = mine * share + start
            out_ref[:, inner] += window_sums(total, haplo_total, first_column, row, ends[:, inner])

        if owner is None:
            add()
        else:
            pl.when(mine == owner)(add)


def early_kernel(share, haplo_total, pieces, ends_ref, *refs):
    out_ref = refs[-1]
    out_ref[...] = jnp.zeros_like(out_ref)
    add_blocks(pieces, refs, share, haplo_total, local_ends(ends_ref, share), out_ref)


def rates_of(share, variants):
    return (math.log(0.5) / (4 * share), math.log(0.1) / variants)


def tail_kernel(share, haplo_total, pieces, rates, ends_ref, sums_ref, decay_ref, *refs):
    score_ref, local_ref, last_ref, total_ref = refs[-4:]
    mine = lax.axis_index("samples")
    ends = local_ends(ends_ref, share)
    total_ref[...] = sums_ref[...]
    add_blocks(pieces, refs, share, haplo_total, ends, total_ref)
    row = mine * share + lax.broadcasted_iota(jnp.int32, (1, share), 1)
    counted = jnp.maximum(ends - row - 1, 1).astype(jnp.float32)
    score = total_ref[...] / counted
    score_ref[...] = score
    blocks = share // LANES
    stacked = jnp.concatenate(
        [score[:, b * LANES : (b + 1) * LANES] for b in range(blocks)]
        + ([jnp.zeros(((-blocks) % 8, LANES), jnp.float32)] if blocks % 8 else []),
        axis=0,
    )
    lane = lax.broadcasted_iota(jnp.int32, (1, LANES), 1).astype(jnp.float32)
    within = lax.dot_general(
        stacked,
        decay_ref[...],
        (((1,), (0,)), ((), ())),
        precision=lax.Precision.HIGHEST,
        preferred_element_type=jnp.float32,
    )
    lasts = []
    for k, rate in enumerate(rates):
        at = 2 * k * LANES
        inner, ending = within[:, at : at + LANES], within[:, at + LANES : at + 2 * LANES]
        fall = jnp.exp((lane + 1.0) * rate)
        block_fall = math.exp(LANES * rate)
        carry = jnp.zeros((1, LANES), jnp.float32)
        for b in range(blocks):
            local_ref[k : k + 1, b * LANES : (b + 1) * LANES] = inner[b : b + 1, :] + carry * fall
            carry = ending[b : b + 1, :] + carry * block_fall
        lasts.append(carry)
    tile_lane = lax.broadcasted_iota(jnp.int32, last_ref.shape, 1)
    last_ref[...] = jnp.where(tile_lane == 0, lasts[0], jnp.where(tile_lane == 1, lasts[1], 0.0))


def finish_kernel(local_ref, table_ref, norm_ref, peer_ref, profile_ref):
    incoming = jnp.sum(peer_ref[...] * table_ref[...], axis=0, keepdims=True)
    for k in range(2):
        profile_ref[k : k + 1, :] = (
            local_ref[k : k + 1, :] * norm_ref[k : k + 1, :]
            + incoming[:, k : k + 1] * norm_ref[2 + k : 3 + k, :]
        )


def peer_constants(rates, share, peers, me):
    f32 = jnp.float32
    log_rates = jnp.array(rates, f32)[:, None]
    step = jnp.arange(share, dtype=jnp.int32)
    position = (me * share + step).astype(f32)[None] + 1.0
    norm = jnp.expm1(log_rates) / jnp.expm1(position * log_rates)
    fall = jnp.exp((step.astype(f32)[None] + 1.0) * log_rates)
    lane = jnp.arange(LANES, dtype=f32)
    lag = lane[None] - lane[:, None]
    decays = []
    for rate in rates:
        decays.append(jnp.where(lag >= 0.0, jnp.exp(jnp.maximum(lag, 0.0) * rate), 0.0))
        decays.append(jnp.broadcast_to(jnp.exp((LANES - 1.0 - lane[:, None]) * rate), lag.shape))
    peer = jnp.arange(peers, dtype=jnp.int32)
    gap = jnp.maximum((me - 1 - peer) * share, 0).astype(f32)
    weight = jnp.where(peer[None] < me, jnp.exp(gap[None] * log_rates), 0.0).T
    weight = jnp.pad(weight, ((0, 0), (0, LANES - len(rates))))
    return jnp.concatenate([norm, norm * fall]), jnp.concatenate(decays, axis=1), weight


def per_device(haplotypes, window_ends):
    samples = lax.axis_size("samples")
    genome = lax.axis_size("genome")
    depth, width = haplotypes.shape
    share = width // samples
    haplo_total = float(depth * samples)
    rates = rates_of(share, width * genome)
    back = [((i + 1) % genome, i) for i in range(genome)]
    ends = window_ends[None]
    f32, bf16 = jnp.float32, jnp.bfloat16
    unit = width // 8
    firsts = [unit * sum(EIGHTHS[:c]) for c in range(len(EIGHTHS))]
    sizes = [unit * e for e in EIGHTHS]

    def shifted(array, c):
        return lax.ppermute(array[:, firsts[c] : firsts[c] + sizes[c]], "genome", back)

    opening = cut(haplotypes, 0, sizes[0])
    raws = [lax.ppermute(opening, "genome", back)]
    haplotypes, counts = load(haplotypes)
    raws += [shifted(haplotypes, c) for c in range(1, len(EIGHTHS))]
    if samples == 2:
        counts = counts + lax.ppermute(counts, "samples", [(0, 1), (1, 0)])
    else:
        counts = lax.psum(counts, "samples")
    next_counts = lax.ppermute(counts, "genome", back)

    def swap(send):
        return lax.ppermute(send, "samples", [(0, 1), (1, 0)])

    tails, tail_pieces = [], []
    token_type = ((8, LANES), f32)
    if samples == 2:
        half, u, whole = share // 2, unit, slice(None)
        standard, norm, decay, peer, token, high, send, low, low_send_1, low_send_2 = call(
            functools.partial(own_kernel, share, haplo_total, rates),
            [((depth, width), bf16), ((4, share), f32), ((LANES, 4 * LANES), f32)]
            + [((genome * samples, LANES), f32), token_type]
            + [((share, share), f32), ((share, share), bf16), ((share, share), f32)]
            + [((half, share), bf16), ((half, half), bf16)],
            haplotypes,
            counts,
        )
        got_0 = swap(send)
        token, keep_1, send = call(
            functools.partial(first_kernel, share, haplo_total),
            [token_type, ((3 * u, share), f32), ((3 * u, share), bf16)],
            raws[0],
            next_counts,
            standard,
            token,
        )
        got_1 = swap(send)
        token, keep_2, send, corner, corner_send = call(
            functools.partial(middle_kernel, firsts[1], share, haplo_total),
            [token_type, ((2 * u, share), f32), ((2 * u, share), bf16), ((u, u), f32), ((u, u), bf16)],
            raws[1],
            next_counts,
            standard,
            low_send_1,
            token,
        )
        got_2 = swap(send)
        first_unit, second_unit = slice(0, u), slice(u, None)
        lower, upper = slice(0, half), slice(half, None)
        tails = [low, corner]
        for c, fills, extra in (
            (2, [(first_unit, lower), (whole, upper)], [low_send_2, corner_send]),
            (3, [(second_unit, lower)], [low_send_2]),
        ):
            shape = (u, width - firsts[c])
            token, keep, send = call(
                functools.partial(upper_kernel, firsts[c], haplo_total, fills),
                [token_type, (shape, f32), (shape, bf16)],
                raws[c],
                next_counts,
                standard,
                token,
                *extra,
            )
            tails += [keep, swap(send)]
        pieces = [
            (None, 0, (whole, whole), 1, (whole, whole), share, 0),
            (None, 2, (whole, whole), 3, (whole, whole), width, 0),
            (0, 4, (slice(half, None), whole), 6, (whole, whole), half, 0),
            (1, 5, (whole, whole), 6, (whole, whole), width + firsts[1], share),
        ]
        (sums,) = call(
            functools.partial(early_kernel, share, haplo_total, pieces),
            [((1, share), f32)],
            ends,
            high,
            got_0,
            keep_1,
            got_1,
            low,
            keep_2,
            got_2,
        )
        keep, send = call(
            functools.partial(last_kernel, firsts[4], haplo_total),
            [((u, u), f32), ((u, u), bf16)],
            raws[4],
            next_counts,
            standard,
        )
        tails += [keep, swap(send)]
        tail_pieces = [
            (0, 0, (first_unit, lower), 3, (whole, lower), 0, 0),
            (0, 0, (slice(u, half), lower), 5, (whole, lower), u, 0),
            (0, 1, (whole, whole), 3, (whole, upper), width + firsts[1], firsts[1]),
        ] + [
            (1, 2 * c - 2, (whole, whole), 2 * c - 1, (whole, whole), width + firsts[c], firsts[c])
            for c in (2, 3, 4)
        ]
    else:
        frequency, inverse_sd = moments(counts, haplo_total)
        standard = standardize(haplotypes, frequency, inverse_sd)
        frequency, inverse_sd = moments(next_counts, haplo_total)
        later = standardize(jnp.concatenate(raws, axis=1), frequency, inverse_sd)
        total = lax.psum_scatter(
            product(jnp.concatenate([standard, later], axis=1), standard),
            "samples",
            scatter_dimension=1,
            tiled=True,
        )
        me = lax.axis_index("genome") * samples + lax.axis_index("samples")
        norm, decay, peer = peer_constants(rates, share, genome * samples, me)
        sums = window_sums(
            total,
            haplo_total,
            0,
            lax.axis_index("samples") * share,
            ends - lax.axis_index("genome") * width,
        )

    score, local, last, _ = call(
        functools.partial(tail_kernel, share, haplo_total, tail_pieces, rates),
        [((1, share), f32), ((2, share), f32), ((genome * samples, LANES), f32), ((1, share), f32)],
        ends,
        sums,
        decay,
        *tails,
    )
    table = lax.all_to_all(last[:, None], ("genome", "samples"), 0, 0, tiled=True)[:, 0]
    (profile,) = call(finish_kernel, [((2, share), f32)], local, table, norm, peer)
    return score[0], profile


def solution(mesh):
    return jax.shard_map(
        per_device,
        mesh=mesh,
        in_specs=(P("samples", "genome"), P(("genome", "samples"))),
        out_specs=(P(("genome", "samples")), P(None, ("genome", "samples"))),
        check_vma=False,
    )
```
